8 devices in a mesh: dp: 1 (over z), ffn: 2 (over y), emb: 4 (over x, core).
Axes of the slice: x: 2, y: 2, z: 1, core: 2. Of those that a mesh axis runs over, the one named last changes fastest.
Arguments:
- hidden: bfloat16 [128, 2048], P('dp', 'emb')
- norm_pre: bfloat16 [2048], P('emb')
- norm_post: bfloat16 [2048], P('emb')
- w_router: bfloat16 [2048, 64], P('emb')
- w_gate: bfloat16 [64, 2048, 1024], P(None, 'emb', 'ffn')
- w_up: bfloat16 [64, 2048, 1024], P(None, 'emb', 'ffn')
- w_down: bfloat16 [64, 1024, 2048], P(None, 'ffn', 'emb')
- choice: int32 [128, 8], P('dp')
Outputs:
- output: bfloat16 [128, 2048], P('dp', 'emb')
All inputs are finite; a program needn't handle non-finite values.
Results may differ from the reference program's by a relative error of at most 0.0126077.
Values are sent between devices in bfloat16 or wider.
A program may use at most 1 GiB of HBM per device.

```python
import math
import jax
import jax.numpy as jnp
from jax import lax

D = 2048
E = 64
F = 1024
TOP = 8
B = 128
CAP = 2 * B * TOP // E
EPS = 1e-5


def width_profile(key, size):
    slope = jax.random.uniform(key, (), minval=1.5, maxval=2.5)
    return jnp.exp(slope * (jnp.arange(size, dtype=jnp.float32) / size - 0.5))


def draw_choice(key):
    key_hot, key_perm, key_score = jax.random.split(key, 3)
    hot_id = jax.random.randint(key_hot, (), 0, E)
    forced = jax.random.permutation(key_perm, B) < (3 * B) // 4
    expert_ids = jnp.arange(E)
    score = jax.random.randint(key_score, (B, E), 1, 1048576) * E + expert_ids[None, :]
    score = jnp.where(forced[:, None] & (expert_ids[None, :] == hot_id), 0, score)
    return jnp.argsort(score, axis=1, stable=True)[:, :TOP].astype(jnp.int32)


def setup_inputs(seed: int = 0, part: int = 0) -> dict:
    base_key = jax.random.key(seed)
    part_keys = jax.random.split(jax.random.fold_in(base_key, part), 4)
    shared_keys = jax.random.split(base_key, 7)
    row_scale = jnp.exp(0.5 * jax.random.normal(part_keys[0], (B, 1)))
    hidden = jax.random.normal(part_keys[1], (B, D)) * row_scale * width_profile(part_keys[2], D)[None, :]
    norm_pre = 1.0 + 0.3 * jax.random.normal(shared_keys[0], (D,))
    norm_post = 1.0 + 0.3 * jax.random.normal(shared_keys[1], (D,))
    w_router = jax.random.normal(shared_keys[2], (D, E)) * (1.5 / math.sqrt(D))
    w_gate = jax.random.normal(shared_keys[3], (E, D, F)) * (1.0 / math.sqrt(D))
    w_up = jax.random.normal(shared_keys[4], (E, D, F)) * (1.0 / math.sqrt(D))
    w_down = jax.random.normal(shared_keys[5], (E, F, D)) * (1.0 / math.sqrt(F)) * width_profile(shared_keys[6], D)[None, None, :]
    return {
        'hidden': hidden.astype(jnp.bfloat16),
        'norm_pre': norm_pre.astype(jnp.bfloat16),
        'norm_post': norm_post.astype(jnp.bfloat16),
        'w_router': w_router.astype(jnp.bfloat16),
        'w_gate': w_gate.astype(jnp.bfloat16),
        'w_up': w_up.astype(jnp.bfloat16),
        'w_down': w_down.astype(jnp.bfloat16),
        'choice': draw_choice(part_keys[3]),
    }


def route_tokens(choice, router_prob):
    onehot = (choice[:, :, None] == jnp.arange(E)[None, None, :]).astype(jnp.int32)
    assigned = jnp.sum(onehot, axis=1)
    before = jnp.cumsum(assigned, axis=0) - assigned
    slot_idx = jnp.sum(onehot * before[:, None, :], axis=2)
    position = jnp.where(slot_idx < CAP, choice * CAP + slot_idx, E * CAP)
    gate_val = jnp.take_along_axis(router_prob, choice, axis=1)
    flat_pos = position.reshape(-1)
    token_ids = jnp.repeat(jnp.arange(B, dtype=jnp.int32), TOP)
    slot_token = jnp.full((E * CAP,), B, jnp.int32).at[flat_pos].set(token_ids, mode='drop')
    slot_gate = jnp.zeros((E * CAP,), jnp.float32).at[flat_pos].set(gate_val.reshape(-1), mode='drop')
    return position, slot_token, slot_gate


def expert_ffn(operands):
    slot_rows, gate_w, up_w, down_w = operands
    z_gate = jnp.dot(slot_rows, gate_w, preferred_element_type=jnp.float32).astype(jnp.bfloat16)
    z_up = jnp.dot(slot_rows, up_w, preferred_element_type=jnp.float32).astype(jnp.bfloat16)
    act_val = (jax.nn.gelu(z_gate.astype(jnp.float32), approximate=True) * z_up.astype(jnp.float32)).astype(jnp.bfloat16)
    return jnp.dot(act_val, down_w, preferred_element_type=jnp.float32).astype(jnp.bfloat16)


def reference(hidden, norm_pre, norm_post, w_router, w_gate, w_up, w_down, choice):
    hid_f32 = hidden.astype(jnp.float32)
    inv_pre = lax.rsqrt(jnp.mean(hid_f32 * hid_f32, axis=1, keepdims=True) + EPS)
    normed = (hid_f32 * inv_pre * norm_pre.astype(jnp.float32)).astype(jnp.bfloat16)
    logits = jnp.dot(normed, w_router, preferred_element_type=jnp.float32)
    router_prob = jax.nn.softmax(logits, axis=1)
    position, slot_token, slot_gate = route_tokens(choice, router_prob)
    expert_in = jnp.take(normed, slot_token, axis=0, mode='fill', fill_value=0).reshape(E, CAP, D)
    expert_out = lax.map(expert_ffn, (expert_in, w_gate, w_up, w_down))
    weighted = (expert_out.reshape(E * CAP, D).astype(jnp.float32) * slot_gate[:, None]).astype(jnp.bfloat16)
    picked = jnp.take(weighted, position, axis=0, mode='fill', fill_value=0)
    mix_sum = jnp.sum(picked.astype(jnp.float32), axis=1)
    inv_post = lax.rsqrt(jnp.mean(mix_sum * mix_sum, axis=1, keepdims=True) + EPS)
    return (hid_f32 + mix_sum * inv_post * norm_post.astype(jnp.float32)).astype(jnp.bfloat16)
```

```python
import functools

import jax
import jax.numpy as jnp
from jax import lax
from jax.experimental import pallas as pl
from jax.experimental.pallas import tpu as pltpu
from jax.sharding import PartitionSpec as P

EPS = 1e-5
MESH = pl.DeviceIdType.MESH
F32 = jnp.float32
BF16 = jnp.bfloat16

CE = 4
NB = 6
NC = 8
LAG_B, LAG_C, LAG_D, LAG_E = 1, 3, 5, 6


def kernel(tok, wid, experts, cap, width, top_k, model_width,
           hid_hbm, pre_ref, post_ref, wr_hbm, wg_hbm, wu_hbm, wd_hbm, ch_hbm, out_ref,
           hid, wr, ch, wg, wu, wd, key, xs, sel, gate, zbuf, rza, sbuf, rzb, gbuf, mix, rmix,
           sqs, sqr, lgs, lgr, sqs2, sqr2,
           small_sem, wg_sem, wu_sem, wd_sem,
           as_sem, ar_sem, bs_sem, br_sem, gcs_sem, gcr_sem, gxs_sem, gxr_sem, gfs_sem, gfr_sem,
           ss_sem, sr_sem, ls_sem, lr_sem, ps_sem, pr_sem, ms_sem, mr_sem):
    nchunk = experts // CE
    rows = CE * cap
    emb = lax.axis_index("emb")
    ffn = lax.axis_index("ffn")
    x, c = emb // 2, emb % 2
    ox, oc = 1 - x, 1 - c
    mate = {"emb": x * 2 + oc}
    across = {"emb": ox * 2 + c}
    diag = {"emb": ox * 2 + oc}
    other = {"ffn": 1 - ffn}
    peers = (mate, across, diag)

    def weight_copies(i):
        s = lax.rem(i, NB)
        e = pl.ds(i * CE, CE)
        return (pltpu.make_async_copy(wg_hbm.at[e], wg.at[s], wg_sem.at[s]),
                pltpu.make_async_copy(wu_hbm.at[e], wu.at[s], wu_sem.at[s]))

    def down_copy(i):
        s = lax.rem(i, NC)
        return pltpu.make_async_copy(wd_hbm.at[pl.ds(i * CE, CE)], wd.at[s], wd_sem.at[s])

    small = (pltpu.make_async_copy(hid_hbm, hid, small_sem.at[0]),
             pltpu.make_async_copy(ch_hbm, ch, small_sem.at[1]),
             pltpu.make_async_copy(wr_hbm, wr, small_sem.at[2]))
    for cp in small:
        cp.start()
    for i in range(NB):
        for cp in weight_copies(i):
            cp.start()

    barrier = pltpu.get_barrier_semaphore()
    for peer in peers + (other,):
        pl.semaphore_signal(barrier, inc=1, device_id=peer, device_id_type=MESH)

    def gather_small(src, dst, send, recv):
        cps = [pltpu.make_async_remote_copy(src, dst.at[j], send.at[j], recv.at[j], device_id=peer, device_id_type=MESH)
               for j, peer in enumerate(peers)]
        for cp in cps:
            cp.start()
        return cps

    def row_sums(sq):
        part = sq[:, 0:128]
        for j in range(1, width // 128):
            part = part + sq[:, j * 128:(j + 1) * 128]
        t = jnp.sum(part.T, axis=0, keepdims=True)
        return jnp.broadcast_to(t, (8, tok))

    def as_row(ref):
        v = ref[...].astype(F32)
        return jnp.concatenate([v[j:j + 1, :] for j in range(width // 128)], axis=1)

    small[0].wait()
    hf = hid[...].astype(F32)
    sqs[...] = row_sums(hf * hf)
    pl.semaphore_wait(barrier, 4)
    sq_cps = gather_small(sqs, sqr, ss_sem, sr_sem)

    small[1].wait()
    expert_id = lax.broadcasted_iota(jnp.int32, (experts, tok), 0)
    chv = ch[...]
    hot = jnp.zeros((experts, tok), F32)
    for k in range(top_k):
        hot = hot + jnp.where(chv[k:k + 1, :] == expert_id, 1.0, 0.0)
    t0 = lax.broadcasted_iota(jnp.int32, (tok, tok), 0)
    t1 = lax.broadcasted_iota(jnp.int32, (tok, tok), 1)
    upper = jnp.where(t0 < t1, 1.0, 0.0).astype(BF16)
    before = jnp.dot(hot.astype(BF16), upper, preferred_element_type=F32)
    key_val = jnp.where((hot > 0.5) & (before < cap - 0.5), before, -1.0)
    dn = (((0,), (0,)), ((), ()))
    slot = lax.broadcasted_iota(jnp.int32, (cap, tok), 0).astype(F32)
    for e in range(experts):
        sel[e * cap:(e + 1) * cap, :] = jnp.where(key_val[e:e + 1, :] == slot, 1.0, 0.0).astype(BF16)

    for cp in sq_cps:
        cp.wait_recv()
    tot = (sqs[0:1, :] + sqr[0, 0:1, :]) + (sqr[1, 0:1, :] + sqr[2, 0:1, :])
    inv = lax.rsqrt(tot / model_width + EPS)
    inv = jnp.broadcast_to(inv, (tok, tok)).T
    inv = jnp.concatenate([inv] * (width // 128), axis=1)
    b = (hf * inv * as_row(pre_ref)).astype(BF16)
    small[2].wait()
    lgs[...] = lax.dot_general(wr[...], b, (((1,), (1,)), ((), ())), preferred_element_type=F32)
    lg_cps = gather_small(lgs, lgr, ls_sem, lr_sem)
    for r in range(0, experts * cap, 256):
        xs[r:r + 256, :] = jnp.dot(sel[r:r + 256, :], b, preferred_element_type=F32).astype(BF16)
    mix[...] = jnp.zeros_like(mix)

    def gates():
        for cp in lg_cps:
            cp.wait_recv()
        lg = (lgs[...] + lgr[0]) + (lgr[1] + lgr[2])
        lg = lg - jnp.max(lg, axis=0, keepdims=True)
        ex = jnp.exp(lg)
        prob = ex / jnp.sum(ex, axis=0, keepdims=True)
        for e in range(experts):
            picked = jnp.where(key_val[e:e + 1, :] == slot, prob[e:e + 1, :], 0.0)
            gate[e * cap:(e + 1) * cap, :] = jnp.broadcast_to(jnp.sum(picked, axis=1, keepdims=True), (cap, 128))

    gates()

    def send_z(i):
        return pltpu.make_async_remote_copy(zbuf.at[i, oc], rza.at[i], as_sem.at[i], ar_sem.at[i],
                                            device_id=mate, device_id_type=MESH)

    def send_s(i):
        return pltpu.make_async_remote_copy(sbuf.at[i], rzb.at[i], bs_sem.at[i], br_sem.at[i],
                                            device_id=across, device_id_type=MESH)

    def send_g(i):
        own = gbuf.at[i, c, x]
        return (pltpu.make_async_remote_copy(own, own, gcs_sem.at[i], gcr_sem.at[i],
                                             device_id=mate, device_id_type=MESH),
                pltpu.make_async_remote_copy(own, own, gxs_sem.at[i], gxr_sem.at[i],
                                             device_id=across, device_id_type=MESH))

    def recv_mate(i):
        z = gbuf.at[i, oc, x]
        return pltpu.make_async_remote_copy(z, z, gcs_sem.at[i], gcr_sem.at[i], device_id=mate, device_id_type=MESH)

    def recv_across(i):
        z = gbuf.at[i, c, ox]
        return pltpu.make_async_remote_copy(z, z, gxs_sem.at[i], gxr_sem.at[i], device_id=across, device_id_type=MESH)

    def forward_g(i):
        z = gbuf.at[i, c, ox]
        return pltpu.make_async_remote_copy(z, z, gfs_sem.at[i], gfr_sem.at[i], device_id=mate, device_id_type=MESH)

    def arrived_g(i):
        z = gbuf.at[i, oc, ox]
        return pltpu.make_async_remote_copy(z, z, gfs_sem.at[i], gfr_sem.at[i], device_id=mate, device_id_type=MESH)

    def stage_a(i):
        s = lax.rem(i, NB)
        for cp in weight_copies(i):
            cp.wait()
        base = pl.multiple_of(i * rows, rows)
        for k in range(CE):
            xe = xs[pl.ds(base + k * cap, cap), :]
            zbuf[i, k // 2, k % 2, :, 0:width] = jnp.dot(xe, wg[s, k], preferred_element_type=F32).astype(BF16)
            zbuf[i, k // 2, k % 2, :, width:2 * width] = jnp.dot(xe, wu[s, k], preferred_element_type=F32).astype(BF16)
        send_z(i).start()

    def refill(i):
        for cp in weight_copies(i):
            cp.start()

    def stage_b(i):
        send_z(i).wait_recv()
        sbuf[i] = (zbuf[i, c, ox].astype(F32) + rza[i, ox].astype(F32)).astype(BF16)
        send_s(i).start()

    def stage_c(i):
        send_s(i).wait_recv()
        z = (zbuf[i, c, x].astype(F32) + rza[i, x].astype(F32) + rzb[i].astype(F32)).astype(BF16).astype(F32)
        act = jax.nn.gelu(z[:, 0:width], approximate=True) * z[:, width:2 * width]
        gbuf[i, c, x] = act.astype(BF16)
        for cp in send_g(i):
            cp.start()

    def stage_d(i):
        recv_across(i).wait_recv()
        forward_g(i).start()

    def stage_e(i):
        s = lax.rem(i, NC)
        down_copy(i).wait()
        recv_mate(i).wait_recv()
        arrived_g(i).wait_recv()
        base = pl.multiple_of(i * rows, rows)
        us = []
        for k in range(CE):
            y = jnp.dot(gbuf[i, k // 2, k % 2], wd[s, k], preferred_element_type=F32).astype(BF16).astype(F32)
            gk = gate[pl.ds(base + k * cap, cap), :]
            us.append((y * jnp.concatenate([gk] * (width // 128), axis=1)).astype(BF16))
        u = jnp.concatenate(us, axis=0)
        mix[...] += lax.dot_general(sel[pl.ds(base, rows), :], u, dn, preferred_element_type=F32)

    def guarded(i):
        pl.when(i >= LAG_B)(lambda: stage_b(i - LAG_B))
        pl.when(i >= LAG_C)(lambda: stage_c(i - LAG_C))
        pl.when(i >= LAG_D)(lambda: stage_d(i - LAG_D))

    @pl.loop(0, LAG_E)
    def _(i):
        down_copy(i).start()
        stage_a(i)
        refill(i + NB)
        guarded(i)

    @pl.loop(LAG_E, nchunk)
    def _(i):
        down_copy(i).start()
        stage_a(i)
        pl.when(i + NB < nchunk)(lambda: refill(i + NB))
        stage_b(i - LAG_B)
        stage_c(i - LAG_C)
        stage_d(i - LAG_D)
        stage_e(i - LAG_E)

    @pl.loop(nchunk, nchunk + LAG_E)
    def _(i):
        pl.when(i - LAG_B < nchunk)(lambda: stage_b(i - LAG_B))
        pl.when(i - LAG_C < nchunk)(lambda: stage_c(i - LAG_C))
        pl.when(i - LAG_D < nchunk)(lambda: stage_d(i - LAG_D))
        stage_e(i - LAG_E)

    mcp = pltpu.make_async_remote_copy(mix, rmix, ms_sem, mr_sem, device_id=other, device_id_type=MESH)
    mcp.start()

    @pl.loop(0, nchunk)
    def _(i):
        send_z(i).wait_send()
        send_s(i).wait_send()
        for cp in send_g(i):
            cp.wait_send()
        forward_g(i).wait_send()

    for cp in sq_cps + lg_cps:
        cp.wait_send()
    mcp.wait()
    m = mix[...] + rmix[...]
    sqs2[...] = row_sums(m * m)
    cps = gather_small(sqs2, sqr2, ps_sem, pr_sem)
    for cp in cps:
        cp.wait()
    tot = (sqs2[0:1, :] + sqr2[0, 0:1, :]) + (sqr2[1, 0:1, :] + sqr2[2, 0:1, :])
    inv = lax.rsqrt(tot / model_width + EPS)
    inv = jnp.broadcast_to(inv, (tok, tok)).T
    inv = jnp.concatenate([inv] * (width // 128), axis=1)
    out_ref[...] = (hid[...].astype(F32) + m * inv * as_row(post_ref)).astype(BF16)


def solution(mesh):
    emb_size = mesh.shape["emb"]

    def local_block(hidden, norm_pre, norm_post, w_router, w_gate, w_up, w_down, choice):
        tok, width = hidden.shape
        experts, _, wid = w_gate.shape
        top_k = choice.shape[1]
        cap = 2 * tok * top_k // experts
        nchunk = experts // CE
        dma = pltpu.SemaphoreType.DMA
        vmem = pltpu.VMEM
        assert emb_size == CE and wid == width
        hbm = pl.BlockSpec(memory_space=pl.ANY)
        vm = pl.BlockSpec(memory_space=pltpu.VMEM)
        return pl.pallas_call(
            functools.partial(kernel, tok, wid, experts, cap, width, top_k, width * emb_size),
            out_shape=jax.ShapeDtypeStruct((tok, width), BF16),
            in_specs=[hbm, vm, vm, hbm, hbm, hbm, hbm, hbm],
            out_specs=vm,
            scratch_shapes=[
                vmem((tok, width), BF16), vmem((experts, width), BF16), vmem((top_k, tok), jnp.int32),
                vmem((NB, CE, width, wid), BF16), vmem((NB, CE, width, wid), BF16), vmem((NC, CE, wid, width), BF16),
                vmem((8, 128), F32),
                vmem((experts * cap, width), BF16), vmem((experts * cap, tok), BF16), vmem((experts * cap, 128), F32),
                vmem((nchunk, 2, 2, cap, 2 * wid), BF16), vmem((nchunk, 2, cap, 2 * wid), BF16),
                vmem((nchunk, cap, 2 * wid), BF16), vmem((nchunk, cap, 2 * wid), BF16),
                vmem((nchunk, 2, 2, cap, wid), BF16),
                vmem((tok, width), F32), vmem((tok, width), F32),
                vmem((8, tok), F32), vmem((3, 8, tok), F32),
                vmem((experts, tok), F32), vmem((3, experts, tok), F32),
                vmem((8, tok), F32), vmem((3, 8, tok), F32),
                dma((3,)), dma((NB,)), dma((NB,)), dma((NC,)),
            ] + [dma((nchunk,))] * 10 + [dma((3,))] * 6 + [dma, dma],
            compiler_params=pltpu.CompilerParams(
                collective_id=0, has_side_effects=True, vmem_limit_bytes=67043328),
        )(hidden, norm_pre.reshape(width // 128, 128), norm_post.reshape(width // 128, 128), w_router.T, w_gate, w_up, w_down, choice.T)

    in_specs = (P("dp", "emb"), P("emb"), P("emb"), P("emb", None), P(None, "emb", "ffn"), P(None, "emb", "ffn"), P(None, "ffn", "emb"), P("dp", None))
    return jax.shard_map(local_block, mesh=mesh, in_specs=in_specs, out_specs=P("dp", "emb"), check_vma=False)
```

```python
import functools

import jax
import jax.numpy as jnp
from jax import lax
from jax.experimental import pallas as pl
from jax.experimental.pallas import tpu as pltpu
from jax.sharding import PartitionSpec as P

EPS = 1e-5
MESH = pl.DeviceIdType.MESH
F32 = jnp.float32
BF16 = jnp.bfloat16

GE = 8
NP = 2
NR = 4


def kernel(tok, wid, experts, cap, width, top_k, model_width,
           hid_hbm, pre_ref, post_ref, wr_hbm, wg_hbm, wu_hbm, wd_hbm, ch_hbm, out_ref,
           hid, wr, ch, wg, wu, wd, xs, sel, dis, gate, zs, zc, rza, rzb, gbuf, mix, rmix,
           sqs, sqr, lgs, lgr, sqs2, sqr2,
           small_sem, wg_sem, wu_sem, wd_sem,
           as_sem, ar_sem, bs_sem, br_sem, gcs_sem, gcr_sem, gxs_sem, gxr_sem, gfs_sem, gfr_sem,
           ss_sem, sr_sem, ls_sem, lr_sem, ps_sem, pr_sem, ms_sem, mr_sem):
    groups = experts // GE
    half = groups // 2
    rows = GE * cap
    quarter = rows // 4
    fw = wid // NP
    emb = lax.axis_index("emb")
    ffn = lax.axis_index("ffn")
    x, c = emb // 2, emb % 2
    ox, oc = 1 - x, 1 - c
    mate = {"emb": x * 2 + oc}
    across = {"emb": ox * 2 + c}
    diag = {"emb": ox * 2 + oc}
    other = {"ffn": 1 - ffn}
    peers = (mate, across, diag)

    def weight_copies(p, g):
        e = pl.ds(g * GE, GE)
        col = pl.ds(p * fw, fw) if isinstance(p, int) else pl.ds(pl.multiple_of(p * fw, fw), fw)
        s = g % NR
        return (pltpu.make_async_copy(wg_hbm.at[e, :, col], wg.at[s], wg_sem.at[s]),
                pltpu.make_async_copy(wu_hbm.at[e, :, col], wu.at[s], wu_sem.at[s]))

    def down_copy(g):
        return pltpu.make_async_copy(wd_hbm.at[pl.ds(g * GE, GE)], wd.at[g], wd_sem.at[g])

    small = (pltpu.make_async_copy(hid_hbm, hid, small_sem.at[0]),
             pltpu.make_async_copy(ch_hbm, ch, small_sem.at[1]),
             pltpu.make_async_copy(wr_hbm, wr, small_sem.at[2]))
    for cp in small:
        cp.start()
    for g in range(NR):
        for cp in weight_copies(0, g):
            cp.start()
    down_copy(0).start()

    barrier = pltpu.get_barrier_semaphore()
    for peer in peers + (other,):
        pl.semaphore_signal(barrier, inc=1, device_id=peer, device_id_type=MESH)

    def gather_small(src, dst, send, recv):
        cps = [pltpu.make_async_remote_copy(src, dst.at[j], send.at[j], recv.at[j], device_id=peer, device_id_type=MESH)
               for j, peer in enumerate(peers)]
        for cp in cps:
            cp.start()
        return cps

    def row_sums(sq):
        part = sq[:, 0:128]
        for j in range(1, width // 128):
            part = part + sq[:, j * 128:(j + 1) * 128]
        t = jnp.sum(part.T, axis=0, keepdims=True)
        return jnp.broadcast_to(t, (8, tok))

    def as_row(ref):
        v = ref[...].astype(F32)
        return jnp.concatenate([v[j:j + 1, :] for j in range(width // 128)], axis=1)

    small[0].wait()
    hf = hid[...].astype(F32)
    sqs[...] = row_sums(hf * hf)
    pl.semaphore_wait(barrier, 4)
    sq_cps = gather_small(sqs, sqr, ss_sem, sr_sem)

    small[1].wait()
    expert_id = lax.broadcasted_iota(jnp.int32, (experts, tok), 0)
    chv = ch[...]
    hot = jnp.zeros((experts, tok), F32)
    for k in range(top_k):
        hot = hot + jnp.where(chv[k:k + 1, :] == expert_id, 1.0, 0.0)
    t0 = lax.broadcasted_iota(jnp.int32, (tok, tok), 0)
    t1 = lax.broadcasted_iota(jnp.int32, (tok, tok), 1)
    upper = jnp.where(t0 < t1, 1.0, 0.0).astype(BF16)
    before = jnp.dot(hot.astype(BF16), upper, preferred_element_type=F32)
    key_val = jnp.where((hot > 0.5) & (before < cap - 0.5), before, -1.0)
    dn = (((0,), (0,)), ((), ()))
    slot = lax.broadcasted_iota(jnp.int32, (cap, tok), 0).astype(F32)
    for e in range(experts):
        sel[e * cap:(e + 1) * cap, :] = jnp.where(key_val[e:e + 1, :] == slot, 1.0, 0.0).astype(BF16)

    filled = jnp.broadcast_to(jnp.minimum(jnp.sum(hot, axis=1, keepdims=True), float(cap)), (experts, 128))
    e0 = lax.broadcasted_iota(jnp.int32, (experts, experts), 0)
    e1 = lax.broadcasted_iota(jnp.int32, (experts, experts), 1)
    lower = jnp.where(e1 < e0, 1.0, 0.0).astype(BF16)
    start = jnp.dot(lower, filled.astype(BF16), preferred_element_type=F32)
    lane = lax.broadcasted_iota(jnp.int32, (cap, 128), 1).astype(F32)
    shift = jnp.zeros((1, 128), F32)
    for g in range(groups):
        base = float(max(0, rows * (g - half)))
        shift = jnp.maximum(shift, base - start[g * GE:g * GE + 1, :])
        for k in range(GE):
            e = g * GE + k
            pos = jnp.where(slot < filled[e:e + 1, :], slot + (start[e:e + 1, :] + shift), -1.0) - lane
            for j in range(half * rows // 128):
                dis[e * cap:(e + 1) * cap, j * 128:(j + 1) * 128] = jnp.where(pos == float(j * 128), 1.0, 0.0).astype(BF16)

    for cp in sq_cps:
        cp.wait_recv()
    tot = (sqs[0:1, :] + sqr[0, 0:1, :]) + (sqr[1, 0:1, :] + sqr[2, 0:1, :])
    inv = lax.rsqrt(tot / model_width + EPS)
    inv = jnp.broadcast_to(inv, (tok, tok)).T
    inv = jnp.concatenate([inv] * (width // 128), axis=1)
    b = (hf * inv * as_row(pre_ref)).astype(BF16)
    small[2].wait()
    lgs[...] = lax.dot_general(wr[...], b, (((1,), (1,)), ((), ())), preferred_element_type=F32)
    lg_cps = gather_small(lgs, lgr, ls_sem, lr_sem)
    for r in range(0, experts * cap, 256):
        xs[r:r + 256, :] = jnp.dot(sel[r:r + 256, :], b, preferred_element_type=F32).astype(BF16)
    mix[...] = jnp.zeros_like(mix)

    def gates():
        for cp in lg_cps:
            cp.wait_recv()
        lg = (lgs[...] + lgr[0]) + (lgr[1] + lgr[2])
        lg = lg - jnp.max(lg, axis=0, keepdims=True)
        ex = jnp.exp(lg)
        prob = ex / jnp.sum(ex, axis=0, keepdims=True)
        for e in range(experts):
            picked = jnp.where(key_val[e:e + 1, :] == slot, prob[e:e + 1, :], 0.0)
            gate[e * cap:(e + 1) * cap, :] = jnp.broadcast_to(jnp.sum(picked, axis=1, keepdims=True), (cap, 128))

    def send_z(i):
        return pltpu.make_async_remote_copy(zc.at[i, oc], rza.at[i], as_sem.at[i], ar_sem.at[i],
                                            device_id=mate, device_id_type=MESH)

    def send_s(i):
        return pltpu.make_async_remote_copy(zc.at[i, c, ox], rzb.at[i], bs_sem.at[i], br_sem.at[i],
                                            device_id=across, device_id_type=MESH)

    def g_copy(i, a, b, send, recv, peer):
        ref = gbuf.at[i, a, b]
        return pltpu.make_async_remote_copy(ref, ref, send.at[i], recv.at[i], device_id=peer, device_id_type=MESH)

    def send_g(i):
        return (g_copy(i, c, x, gcs_sem, gcr_sem, mate), g_copy(i, c, x, gxs_sem, gxr_sem, across))

    def recv_mate(i):
        return g_copy(i, oc, x, gcs_sem, gcr_sem, mate)

    def recv_across(i):
        return g_copy(i, c, ox, gxs_sem, gxr_sem, across)

    def forward_g(i):
        return g_copy(i, c, ox, gfs_sem, gfr_sem, mate)

    def recv_forward(i):
        return g_copy(i, oc, ox, gfs_sem, gfr_sem, mate)

    def stage_a(p, g):
        s = g % NR
        for cp in weight_copies(p, g):
            cp.wait()
        for k in range(GE):
            r = (g * GE + k) * cap
            xe = xs[r:r + cap, :]
            zs[r:r + cap, 0:fw] = jnp.dot(xe, wg[s, k], preferred_element_type=F32).astype(BF16)
            zs[r:r + cap, fw:2 * fw] = jnp.dot(xe, wu[s, k], preferred_element_type=F32).astype(BF16)

    def compact(i, k):
        depth = rows * (half + 1 + k)
        z = lax.dot_general(dis[0:depth, k * rows:(k + 1) * rows], zs[0:depth, :], dn,
                            preferred_element_type=F32).astype(BF16)
        for q in range(4):
            zc[i, q // 2, q % 2] = z[q * quarter:(q + 1) * quarter]
        send_z(i).start()

    def stage_b(i):
        send_z(i).wait_recv()
        zc[i, c, ox] = (zc[i, c, ox].astype(F32) + rza[i, ox].astype(F32)).astype(BF16)
        send_s(i).start()

    def stage_c(i):
        send_s(i).wait_recv()
        z = (zc[i, c, x].astype(F32) + rza[i, x].astype(F32) + rzb[i].astype(F32)).astype(BF16).astype(F32)
        act = jax.nn.gelu(z[:, 0:fw], approximate=True) * z[:, fw:2 * fw]
        gbuf[i, c, x] = act.astype(BF16)
        for cp in send_g(i):
            cp.start()

    def stage_d(i):
        recv_across(i).wait_recv()
        forward_g(i).start()

    def arrived(i):
        recv_mate(i).wait_recv()
        recv_forward(i).wait_recv()

    def stage_e(g):
        down_copy(g).wait()
        nblk = min(g + 1, half)
        depth = nblk * rows
        d = dis[g * rows:(g + 1) * rows, 0:depth]
        gs = [jnp.dot(d, gbuf[p * half:p * half + nblk].reshape(depth, fw), preferred_element_type=F32).astype(BF16)
              for p in range(NP)]
        gs = jnp.concatenate(gs, axis=1)
        us = []
        for k in range(GE):
            r = (g * GE + k) * cap
            y = jnp.dot(gs[k * cap:(k + 1) * cap], wd[g, k], preferred_element_type=F32).astype(BF16).astype(F32)
            gk = gate[r:r + cap, :]
            us.append((y * jnp.concatenate([gk] * (width // 128), axis=1)).astype(BF16))
        u = jnp.concatenate(us, axis=0)
        mix[...] += lax.dot_general(sel[g * rows:(g + 1) * rows, :], u, dn, preferred_element_type=F32)

    @pl.loop(0, NP)
    def _(p):
        first = p * half
        prev = first - half
        later = p > 0
        for g in range(groups):
            stage_a(p, g)
            if g < NR:
                for cp in weight_copies(p, g + NR):
                    cp.start()
            else:
                @pl.when(p == 0)
                def _():
                    for cp in weight_copies(1, g - NR):
                        cp.start()

                @pl.when(p == NP - 1)
                def _():
                    for h in (2 * (g - NR) + 1, 2 * (g - NR) + 2):
                        if h < groups:
                            down_copy(h).start()
            if g >= half:
                compact(first + g - half, g - half)
            if g > half:
                stage_b(first + g - half - 1)

            @pl.when(later)
            def _():
                if g == 0:
                    stage_b(prev + 3)
                    stage_c(prev)
                if g == 1:
                    gates()
                    stage_c(prev + 1)
                if g == 3:
                    stage_c(prev + 2)
                if g == 5:
                    stage_c(prev + 3)
                if g >= 4:
                    stage_d(prev + g - 4)

    last = (NP - 1) * half
    stage_b(last + 3)
    stage_c(last)
    stage_c(last + 1)
    for i in range(last):
        arrived(i)
    stage_d(last)
    stage_c(last + 2)
    arrived(last)
    stage_e(0)
    stage_d(last + 1)
    stage_c(last + 3)
    arrived(last + 1)
    stage_e(1)
    stage_d(last + 2)
    arrived(last + 2)
    stage_e(2)
    stage_d(last + 3)
    arrived(last + 3)
    for g in range(3, groups):
        stage_e(g)

    mcp = pltpu.make_async_remote_copy(mix, rmix, ms_sem, mr_sem, device_id=other, device_id_type=MESH)
    mcp.start()

    for i in range(NP * half):
        send_z(i).wait_send()
        send_s(i).wait_send()
        for cp in send_g(i):
            cp.wait_send()
        forward_g(i).wait_send()
    for cp in sq_cps + lg_cps:
        cp.wait_send()
    mcp.wait()
    m = mix[...] + rmix[...]
    sqs2[...] = row_sums(m * m)
    cps = gather_small(sqs2, sqr2, ps_sem, pr_sem)
    for cp in cps:
        cp.wait()
    tot = (sqs2[0:1, :] + sqr2[0, 0:1, :]) + (sqr2[1, 0:1, :] + sqr2[2, 0:1, :])
    inv = lax.rsqrt(tot / model_width + EPS)
    inv = jnp.broadcast_to(inv, (tok, tok)).T
    inv = jnp.concatenate([inv] * (width // 128), axis=1)
    out_ref[...] = (hid[...].astype(F32) + m * inv * as_row(post_ref)).astype(BF16)


def solution(mesh):
    emb_size = mesh.shape["emb"]

    def local_block(hidden, norm_pre, norm_post, w_router, w_gate, w_up, w_down, choice):
        tok, width = hidden.shape
        experts, _, wid = w_gate.shape
        top_k = choice.shape[1]
        cap = 2 * tok * top_k // experts
        groups = experts // GE
        nblk = NP * groups // 2
        slots, quarter, fw = experts * cap, GE * cap // 4, wid // NP
        dma = pltpu.SemaphoreType.DMA
        vmem = pltpu.VMEM
        assert emb_size == 4 and wid == width and slots == 2 * tok * top_k
        hbm = pl.BlockSpec(memory_space=pl.ANY)
        vm = pl.BlockSpec(memory_space=pltpu.VMEM)
        return pl.pallas_call(
            functools.partial(kernel, tok, wid, experts, cap, width, top_k, width * emb_size),
            out_shape=jax.ShapeDtypeStruct((tok, width), BF16),
            in_specs=[hbm, vm, vm, hbm, hbm, hbm, hbm, hbm],
            out_specs=vm,
            scratch_shapes=[
                vmem((tok, width), BF16), vmem((experts, width), BF16), vmem((top_k, tok), jnp.int32),
                vmem((NR, GE, width, fw), BF16), vmem((NR, GE, width, fw), BF16), vmem((groups, GE, wid, width), BF16),
                vmem((slots, width), BF16), vmem((slots, tok), BF16), vmem((slots, slots // 2), BF16), vmem((slots, 128), F32),
                vmem((slots, 2 * fw), BF16), vmem((nblk, 2, 2, quarter, 2 * fw), BF16), vmem((nblk, 2, quarter, 2 * fw), BF16),
                vmem((nblk, quarter, 2 * fw), BF16),
                vmem((nblk, 2, 2, quarter, fw), BF16),
                vmem((tok, width), F32), vmem((tok, width), F32),
                vmem((8, tok), F32), vmem((3, 8, tok), F32),
                vmem((experts, tok), F32), vmem((3, experts, tok), F32),
                vmem((8, tok), F32), vmem((3, 8, tok), F32),
                dma((3,)), dma((NR,)), dma((NR,)), dma((groups,)),
            ] + [dma((nblk,))] * 10 + [dma((3,))] * 6 + [dma, dma],
            compiler_params=pltpu.CompilerParams(
                collective_id=0, has_side_effects=True, vmem_limit_bytes=67043328),
        )(hidden, norm_pre.reshape(width // 128, 128), norm_post.reshape(width // 128, 128), w_router.T, w_gate, w_up, w_down, choice.T)

    in_specs = (P("dp", "emb"), P("emb"), P("emb"), P("emb", None), P(None, "emb", "ffn"), P(None, "emb", "ffn"), P(None, "ffn", "emb"), P("dp", None))
    return jax.shard_map(local_block, mesh=mesh, in_specs=in_specs, out_specs=P("dp", "emb"), check_vma=False)
```

```python
import functools

import jax
import jax.numpy as jnp
from jax import lax
from jax.experimental import pallas as pl
from jax.experimental.pallas import tpu as pltpu
from jax.sharding import PartitionSpec as P

EPS = 1e-5
MESH = pl.DeviceIdType.MESH
F32 = jnp.float32
BF16 = jnp.bfloat16

GE = 8
NP = 2
NR = 3


def kernel(tok, wid, experts, cap, width, top_k, model_width,
           hid_hbm, pre_ref, post_ref, wr_hbm, wg_hbm, wu_hbm, wd_hbm, ch_hbm, out_ref,
           hid, wr, ch, wg, wu, wd, xs, sel, dis, gate, zs, zc, rza, rzb, gbuf, y0, mix, rmix,
           sqs, sqr, lgs, lgr, sqs2, sqr2,
           small_sem, wg_sem, wu_sem, wd_sem,
           as_sem, ar_sem, bs_sem, br_sem, gcs_sem, gcr_sem, gxs_sem, gxr_sem, gfs_sem, gfr_sem,
           ss_sem, sr_sem, ls_sem, lr_sem, ps_sem, pr_sem, ms_sem, mr_sem):
    groups = experts // GE
    half = groups // 2
    rows = GE * cap
    quarter = rows // 4
    fw = wid // NP
    emb = lax.axis_index("emb")
    ffn = lax.axis_index("ffn")
    x, c = emb // 2, emb % 2
    ox, oc = 1 - x, 1 - c
    mate = {"emb": x * 2 + oc}
    across = {"emb": ox * 2 + c}
    diag = {"emb": ox * 2 + oc}
    other = {"ffn": 1 - ffn}
    peers = (mate, across, diag)

    def weight_copies(p, g):
        e = pl.ds(g * GE, GE)
        col = pl.ds(p * fw, fw)
        s = (p * groups + g) % NR
        return (pltpu.make_async_copy(wg_hbm.at[e, :, col], wg.at[s], wg_sem.at[s]),
                pltpu.make_async_copy(wu_hbm.at[e, :, col], wu.at[s], wu_sem.at[s]))

    def down_copy(g):
        return pltpu.make_async_copy(wd_hbm.at[pl.ds(g * GE, GE)], wd.at[g], wd_sem.at[g])

    small = (pltpu.make_async_copy(hid_hbm, hid, small_sem.at[0]),
             pltpu.make_async_copy(ch_hbm, ch, small_sem.at[1]),
             pltpu.make_async_copy(wr_hbm, wr, small_sem.at[2]))
    for cp in small:
        cp.start()
    barrier = pltpu.get_barrier_semaphore()
    for peer in peers + (other,):
        pl.semaphore_signal(barrier, inc=1, device_id=peer, device_id_type=MESH)

    def gather_small(src, dst, send, recv):
        cps = [pltpu.make_async_remote_copy(src, dst.at[j], send.at[j], recv.at[j], device_id=peer, device_id_type=MESH)
               for j, peer in enumerate(peers)]
        for cp in cps:
            cp.start()
        return cps

    def row_sums(sq):
        part = sq[:, 0:128]
        for j in range(1, width // 128):
            part = part + sq[:, j * 128:(j + 1) * 128]
        t = jnp.sum(part.T, axis=0, keepdims=True)
        return jnp.broadcast_to(t, (8, tok))

    def as_row(ref):
        v = ref[...].astype(F32)
        return jnp.concatenate([v[j:j + 1, :] for j in range(width // 128)], axis=1)

    for cp in small:
        cp.wait()
    for g in range(NR):
        for cp in weight_copies(0, g):
            cp.start()
    down_copy(0).start()
    down_copy(1).start()
    hf = hid[...].astype(F32)
    sqs[...] = row_sums(hf * hf)
    pl.semaphore_wait(barrier, 4)
    sq_cps = gather_small(sqs, sqr, ss_sem, sr_sem)

    expert_id = lax.broadcasted_iota(jnp.int32, (experts, tok), 0)
    chv = ch[...]
    hot = jnp.zeros((experts, tok), F32)
    for k in range(top_k):
        hot = hot + jnp.where(chv[k:k + 1, :] == expert_id, 1.0, 0.0)
    t0 = lax.broadcasted_iota(jnp.int32, (tok, tok), 0)
    t1 = lax.broadcasted_iota(jnp.int32, (tok, tok), 1)
    upper = jnp.where(t0 < t1, 1.0, 0.0).astype(BF16)
    before = jnp.dot(hot.astype(BF16), upper, preferred_element_type=F32)
    key_val = jnp.where((hot > 0.5) & (before < cap - 0.5), before, -1.0)
    dn = (((0,), (0,)), ((), ()))
    slot = lax.broadcasted_iota(jnp.int32, (cap, tok), 0).astype(F32)
    for e in range(experts):
        sel[e * cap:(e + 1) * cap, :] = jnp.where(key_val[e:e + 1, :] == slot, 1.0, 0.0).astype(BF16)

    filled = jnp.broadcast_to(jnp.minimum(jnp.sum(hot, axis=1, keepdims=True), float(cap)), (experts, 128))
    e0 = lax.broadcasted_iota(jnp.int32, (experts, experts), 0)
    e1 = lax.broadcasted_iota(jnp.int32, (experts, experts), 1)
    lower = jnp.where(e1 < e0, 1.0, 0.0).astype(BF16)
    start = jnp.dot(lower, filled.astype(BF16), preferred_element_type=F32)
    lane = lax.broadcasted_iota(jnp.int32, (cap, 128), 1).astype(F32)
    shift = jnp.zeros((1, 128), F32)
    for g in range(groups):
        base = float(max(0, rows * (g - half)))
        shift = jnp.maximum(shift, base - start[g * GE:g * GE + 1, :])
        for k in range(GE):
            e = g * GE + k
            pos = jnp.where(slot < filled[e:e + 1, :], slot + (start[e:e + 1, :] + shift), -1.0) - lane
            for j in range(half * rows // 128):
                dis[e * cap:(e + 1) * cap, j * 128:(j + 1) * 128] = jnp.where(pos == float(j * 128), 1.0, 0.0).astype(BF16)

    for cp in sq_cps:
        cp.wait_recv()
    tot = (sqs[0:1, :] + sqr[0, 0:1, :]) + (sqr[1, 0:1, :] + sqr[2, 0:1, :])
    inv = lax.rsqrt(tot / model_width + EPS)
    inv = jnp.broadcast_to(inv, (tok, tok)).T
    inv = jnp.concatenate([inv] * (width // 128), axis=1)
    b = (hf * inv * as_row(pre_ref)).astype(BF16)
    lgs[...] = lax.dot_general(wr[...], b, (((1,), (1,)), ((), ())), preferred_element_type=F32)
    lg_cps = gather_small(lgs, lgr, ls_sem, lr_sem)
    def dispatch(g):
        r = g * rows
        xs[r:r + rows, :] = jnp.dot(sel[r:r + rows, :], b, preferred_element_type=F32).astype(BF16)

    dispatch(0)
    mix[...] = jnp.zeros_like(mix)

    def gates():
        lg = (lgs[...] + lgr[0]) + (lgr[1] + lgr[2])
        lg = lg - jnp.max(lg, axis=0, keepdims=True)
        ex = jnp.exp(lg)
        prob = ex / jnp.sum(ex, axis=0, keepdims=True)
        for e in range(experts):
            picked = jnp.where(key_val[e:e + 1, :] == slot, prob[e:e + 1, :], 0.0)
            gate[e * cap:(e + 1) * cap, :] = jnp.broadcast_to(jnp.sum(picked, axis=1, keepdims=True), (cap, 128))

    def send_z(i):
        return pltpu.make_async_remote_copy(zc.at[i, oc], rza.at[i], as_sem.at[i], ar_sem.at[i],
                                            device_id=mate, device_id_type=MESH)

    def send_s(i):
        return pltpu.make_async_remote_copy(zc.at[i, c, ox], rzb.at[i], bs_sem.at[i], br_sem.at[i],
                                            device_id=across, device_id_type=MESH)

    def g_copy(i, a, b, send, recv, peer):
        ref = gbuf.at[i, a, b]
        return pltpu.make_async_remote_copy(ref, ref, send.at[i], recv.at[i], device_id=peer, device_id_type=MESH)

    def send_g(i):
        return (g_copy(i, c, x, gcs_sem, gcr_sem, mate), g_copy(i, c, x, gxs_sem, gxr_sem, across))

    def recv_mate(i):
        return g_copy(i, oc, x, gcs_sem, gcr_sem, mate)

    def recv_across(i):
        return g_copy(i, c, ox, gxs_sem, gxr_sem, across)

    def forward_g(i):
        return g_copy(i, c, ox, gfs_sem, gfr_sem, mate)

    def recv_forward(i):
        return g_copy(i, oc, ox, gfs_sem, gfr_sem, mate)

    def stage_a(p, g):
        s = (p * groups + g) % NR
        for k in range(GE):
            r = (g * GE + k) * cap
            xe = xs[r:r + cap, :]
            zs[r:r + cap, 0:fw] = jnp.dot(xe, wg[s, k], preferred_element_type=F32).astype(BF16)
            zs[r:r + cap, fw:2 * fw] = jnp.dot(xe, wu[s, k], preferred_element_type=F32).astype(BF16)

    def compact(i):
        k = i % half
        lo, hi = k * rows, (k + half + 1) * rows
        z = lax.dot_general(dis[lo:hi, k * rows:(k + 1) * rows], zs[lo:hi, :], dn,
                            preferred_element_type=F32).astype(BF16)
        for q in range(4):
            zc[i, q // 2, q % 2] = z[q * quarter:(q + 1) * quarter]
        send_z(i).start()

    def stage_b(i):
        zc[i, c, ox] = (zc[i, c, ox].astype(F32) + rza[i, ox].astype(F32)).astype(BF16)
        send_s(i).start()

    def stage_c(i):
        z = (zc[i, c, x].astype(F32) + rza[i, x].astype(F32) + rzb[i].astype(F32)).astype(BF16).astype(F32)
        act = jax.nn.gelu(z[:, 0:fw], approximate=True) * z[:, fw:2 * fw]
        gbuf[i, c, x] = act.astype(BF16)
        for cp in send_g(i):
            cp.start()

    def exchange(b_list, c_list, d_list):
        for i in b_list:
            send_z(i).wait_recv()
        for i in c_list:
            send_s(i).wait_recv()
        for i in d_list:
            recv_across(i).wait_recv()
        for i in b_list:
            stage_b(i)
        for i in c_list:
            stage_c(i)
        for i in d_list:
            forward_g(i).start()

    def arrived(i):
        recv_mate(i).wait_recv()
        recv_forward(i).wait_recv()

    def undo(p, g):
        lo, hi = max(0, g - half), min(g + 1, half)
        act = gbuf[p * half + lo:p * half + hi].reshape((hi - lo) * rows, fw)
        return jnp.dot(dis[g * rows:(g + 1) * rows, lo * rows:hi * rows], act, preferred_element_type=F32).astype(BF16)

    def down_first(g):
        gs = undo(0, g)
        for k in range(GE):
            r = (g * GE + k) * cap
            y0[r:r + cap, :] = jnp.dot(gs[k * cap:(k + 1) * cap], wd[g, k, 0:fw, :], preferred_element_type=F32)

    def down_last(g, h, gs):
        cols = slice(h * hw, (h + 1) * hw)
        us = []
        for k in range(GE):
            r = (g * GE + k) * cap
            y = y0[r:r + cap, cols] + jnp.dot(gs[k * cap:(k + 1) * cap], wd[g, k, fw:2 * fw, cols], preferred_element_type=F32)
            gk = gate[r:r + cap, :]
            us.append((y.astype(BF16).astype(F32) * jnp.concatenate([gk] * (hw // 128), axis=1)).astype(BF16))
        u = jnp.concatenate(us, axis=0)
        mix[h] += lax.dot_general(sel[g * rows:(g + 1) * rows, :], u, dn, preferred_element_type=F32)

    def down_both(g):
        gs = undo(1, g)
        for h in range(2):
            down_last(g, h, gs)

    hw = width // 2
    b_at, c_at, d_at = {7: (0,), 8: (1,), 9: (2,), 10: (3,), 14: (4,), 15: (5,)}, {10: (0,), 11: (1,), 12: (2,), 13: (3,)}, {14: (0,), 15: (1,)}
    for t in range(NP * groups):
        p, g = divmod(t, groups)
        for cp in weight_copies(p, g):
            cp.wait()
        if t == 3:
            for cp in lg_cps:
                cp.wait_recv()
        exchange(b_at.get(t, ()), c_at.get(t, ()), d_at.get(t, ()))
        if g > half:
            compact(p * half + g - half - 1)
        elif g == 0 and p > 0:
            compact(p * half - 1)
        stage_a(p, g)
        if p == 0 and g + 1 < groups:
            dispatch(g + 1)
        if t == 3:
            gates()
        if t + NR < NP * groups:
            for cp in weight_copies(*divmod(t + NR, groups)):
                cp.start()
        elif t + NR < NP * groups + 2:
            down_copy(t + NR - NP * groups + 2).start()
        else:
            for h in range(4, groups):
                down_copy(h).start()

    exchange((6,), (), (2, 3))
    compact(7)
    down_copy(0).wait()
    arrived(0)
    down_first(0)
    exchange((7,), (4,), ())
    arrived(1)
    arrived(2)
    down_copy(1).wait()
    down_copy(2).wait()
    down_first(1)
    down_first(2)
    exchange((), (5,), ())
    arrived(3)
    down_copy(3).wait()
    down_first(3)
    exchange((), (6,), ())
    down_copy(4).wait()
    down_first(4)
    exchange((), (7,), ())
    down_copy(5).wait()
    down_first(5)
    exchange((), (), (4,))
    exchange((), (), (5,))
    down_copy(6).wait()
    down_first(6)
    exchange((), (), (6,))
    arrived(4)
    down_both(0)
    exchange((), (), (7,))
    arrived(5)
    down_both(1)
    down_copy(7).wait()
    down_first(7)
    arrived(6)
    down_both(2)
    arrived(7)
    for h in range(2):
        for g in range(3, groups):
            r = g * rows
            if h == 0:
                zs[r:r + rows, 0:fw] = undo(1, g)
            down_last(g, h, zs[r:r + rows, 0:fw])
        pltpu.make_async_remote_copy(mix.at[h], rmix.at[h], ms_sem.at[h], mr_sem.at[h],
                                     device_id=other, device_id_type=MESH).start()

    for i in range(NP * half):
        send_z(i).wait_send()
        send_s(i).wait_send()
        for cp in send_g(i):
            cp.wait_send()
        forward_g(i).wait_send()
    for cp in sq_cps + lg_cps:
        cp.wait_send()
    ms = []
    for h in range(2):
        pltpu.make_async_remote_copy(mix.at[h], rmix.at[h], ms_sem.at[h], mr_sem.at[h],
                                     device_id=other, device_id_type=MESH).wait()
        ms.append(mix[h] + rmix[h])
    m = jnp.concatenate(ms, axis=1)
    sqs2[...] = row_sums(m * m)
    cps = gather_small(sqs2, sqr2, ps_sem, pr_sem)
    for cp in cps:
        cp.wait()
    tot = (sqs2[0:1, :] + sqr2[0, 0:1, :]) + (sqr2[1, 0:1, :] + sqr2[2, 0:1, :])
    inv = lax.rsqrt(tot / model_width + EPS)
    inv = jnp.broadcast_to(inv, (tok, tok)).T
    inv = jnp.concatenate([inv] * (width // 128), axis=1)
    out_ref[...] = (hid[...].astype(F32) + m * inv * as_row(post_ref)).astype(BF16)


def solution(mesh):
    emb_size = mesh.shape["emb"]

    def local_block(hidden, norm_pre, norm_post, w_router, w_gate, w_up, w_down, choice):
        tok, width = hidden.shape
        experts, _, wid = w_gate.shape
        top_k = choice.shape[1]
        cap = 2 * tok * top_k // experts
        groups = experts // GE
        nblk = NP * groups // 2
        slots, quarter, fw = experts * cap, GE * cap // 4, wid // NP
        dma = pltpu.SemaphoreType.DMA
        vmem = pltpu.VMEM
        assert emb_size == 4 and wid == width and slots == 2 * tok * top_k
        hbm = pl.BlockSpec(memory_space=pl.ANY)
        vm = pl.BlockSpec(memory_space=pltpu.VMEM)
        return pl.pallas_call(
            functools.partial(kernel, tok, wid, experts, cap, width, top_k, width * emb_size),
            out_shape=jax.ShapeDtypeStruct((tok, width), BF16),
            in_specs=[hbm, vm, vm, hbm, hbm, hbm, hbm, hbm],
            out_specs=vm,
            scratch_shapes=[
                vmem((tok, width), BF16), vmem((experts, width), BF16), vmem((top_k, tok), jnp.int32),
                vmem((NR, GE, width, fw), BF16), vmem((NR, GE, width, fw), BF16), vmem((groups, GE, wid, width), BF16),
                vmem((slots, width), BF16), vmem((slots, tok), BF16), vmem((slots, slots // 2), BF16), vmem((slots, 128), F32),
                vmem((slots, 2 * fw), BF16), vmem((nblk, 2, 2, quarter, 2 * fw), BF16), vmem((nblk, 2, quarter, 2 * fw), BF16),
                vmem((nblk, quarter, 2 * fw), BF16),
                vmem((nblk, 2, 2, quarter, fw), BF16),
                vmem((slots, width), F32), vmem((2, tok, width // 2), F32), vmem((2, tok, width // 2), F32),
                vmem((8, tok), F32), vmem((3, 8, tok), F32),
                vmem((experts, tok), F32), vmem((3, experts, tok), F32),
                vmem((8, tok), F32), vmem((3, 8, tok), F32),
                dma((3,)), dma((NR,)), dma((NR,)), dma((groups,)),
            ] + [dma((nblk,))] * 10 + [dma((3,))] * 6 + [dma((2,))] * 2,
            compiler_params=pltpu.CompilerParams(
                collective_id=0, has_side_effects=True, vmem_limit_bytes=67043328),
        )(hidden, norm_pre.reshape(width // 128, 128), norm_post.reshape(width // 128, 128), w_router.T, w_gate, w_up, w_down, choice.T)

    in_specs = (P("dp", "emb"), P("emb"), P("emb"), P("emb", None), P(None, "emb", "ffn"), P(None, "emb", "ffn"), P(None, "ffn", "emb"), P("dp", None))
    return jax.shard_map(local_block, mesh=mesh, in_specs=in_specs, out_specs=P("dp", "emb"), check_vma=False)
```

```python
import functools

import jax
import jax.numpy as jnp
from jax import lax
from jax.experimental import pallas as pl
from jax.experimental.pallas import tpu as pltpu
from jax.sharding import PartitionSpec as P

EPS = 1e-5
MESH = pl.DeviceIdType.MESH
F32 = jnp.float32
BF16 = jnp.bfloat16

GE = 8
NP = 2
NR = 3
WIN = 48


def kernel(tok, wid, experts, cap, width, top_k, model_width,
           hid_hbm, pre_ref, post_ref, wr_hbm, wg_hbm, wu_hbm, wd_hbm, ch_hbm, out_ref,
           hid, wr, ch, wg, wu, wd, xs, sel, dis, keyw, probs, selw, gate, posv, poss, zs, zc, rza, rzb, gbuf, act, mix, rmix,
           sqs, sqr, lgs, lgr, sqs2, sqr2,
           small_sem, pos_sem, wg_sem, wu_sem, wd_sem,
           as_sem, ar_sem, bs_sem, br_sem, gcs_sem, gcr_sem, gxs_sem, gxr_sem, gfs_sem, gfr_sem,
           ss_sem, sr_sem, ls_sem, lr_sem, ps_sem, pr_sem, ms_sem, mr_sem):
    groups = experts // GE
    half = groups // 2
    rows = GE * cap
    slots = experts * cap
    quarter = rows // 4
    fw = wid // NP
    emb = lax.axis_index("emb")
    ffn = lax.axis_index("ffn")
    x, c = emb // 2, emb % 2
    ox, oc = 1 - x, 1 - c
    mate = {"emb": x * 2 + oc}
    across = {"emb": ox * 2 + c}
    diag = {"emb": ox * 2 + oc}
    other = {"ffn": 1 - ffn}
    peers = (mate, across, diag)

    def weight_copies(p, g):
        e = pl.ds(g * GE, GE)
        col = pl.ds(p * fw, fw)
        s = (p * groups + g) % NR
        return (pltpu.make_async_copy(wg_hbm.at[e, :, col], wg.at[s], wg_sem.at[s]),
                pltpu.make_async_copy(wu_hbm.at[e, :, col], wu.at[s], wu_sem.at[s]))

    def down_copy(g):
        return pltpu.make_async_copy(wd_hbm.at[pl.ds(g * GE, GE)], wd.at[g], wd_sem.at[g])

    small = (pltpu.make_async_copy(hid_hbm, hid, small_sem.at[0]),
             pltpu.make_async_copy(ch_hbm, ch, small_sem.at[1]),
             pltpu.make_async_copy(wr_hbm, wr, small_sem.at[2]))
    for cp in small:
        cp.start()
    barrier = pltpu.get_barrier_semaphore()
    for peer in peers + (other,):
        pl.semaphore_signal(barrier, inc=1, device_id=peer, device_id_type=MESH)

    def gather_small(src, dst, send, recv):
        cps = [pltpu.make_async_remote_copy(src, dst.at[j], send.at[j], recv.at[j], device_id=peer, device_id_type=MESH)
               for j, peer in enumerate(peers)]
        for cp in cps:
            cp.start()
        return cps

    def row_sums(sq):
        part = sq[:, 0:128]
        for j in range(1, width // 128):
            part = part + sq[:, j * 128:(j + 1) * 128]
        t = jnp.sum(part.T, axis=0, keepdims=True)
        return jnp.broadcast_to(t, (8, tok))

    def as_row(ref):
        v = ref[...].astype(F32)
        return jnp.concatenate([v[j:j + 1, :] for j in range(width // 128)], axis=1)

    for cp in small:
        cp.wait()
    for g in range(NR):
        for cp in weight_copies(0, g):
            cp.start()
    down_copy(0).start()
    down_copy(1).start()
    hf = hid[...].astype(F32)
    sqs[...] = row_sums(hf * hf)
    pl.semaphore_wait(barrier, 4)
    sq_cps = gather_small(sqs, sqr, ss_sem, sr_sem)

    expert_id = lax.broadcasted_iota(jnp.int32, (experts, tok), 0)
    chv = ch[...]
    hot = jnp.zeros((experts, tok), F32)
    for k in range(top_k):
        hot = hot + jnp.where(chv[k:k + 1, :] == expert_id, 1.0, 0.0)
    t0 = lax.broadcasted_iota(jnp.int32, (tok, tok), 0)
    t1 = lax.broadcasted_iota(jnp.int32, (tok, tok), 1)
    upper = jnp.where(t0 < t1, 1.0, 0.0).astype(BF16)
    before = jnp.dot(hot.astype(BF16), upper, preferred_element_type=F32)
    key_val = jnp.where((hot > 0.5) & (before < cap - 0.5), before, -1.0)
    dn = (((0,), (0,)), ((), ()))
    slot = lax.broadcasted_iota(jnp.int32, (cap, tok), 0).astype(F32)
    for e in range(experts):
        sel[e * cap:(e + 1) * cap, :] = jnp.where(key_val[e:e + 1, :] == slot, 1.0, 0.0).astype(BF16)

    filled = jnp.broadcast_to(jnp.minimum(jnp.sum(hot, axis=1, keepdims=True), float(cap)), (experts, 128))
    e0 = lax.broadcasted_iota(jnp.int32, (experts, experts), 0)
    e1 = lax.broadcasted_iota(jnp.int32, (experts, experts), 1)
    lower = jnp.where(e1 < e0, 1.0, 0.0).astype(BF16)
    start = jnp.dot(lower, filled.astype(BF16), preferred_element_type=F32)
    lane = lax.broadcasted_iota(jnp.int32, (cap, 128), 1).astype(F32)
    shift = jnp.zeros((1, 128), F32)
    place = []
    for g in range(groups):
        base = float(max(0, rows * (g - half)))
        shift = jnp.maximum(shift, base - start[g * GE:g * GE + 1, :])
        place.append(start[g * GE:(g + 1) * GE, :] + shift)
    place = jnp.concatenate(place, axis=0)
    for e in range(experts):
        pos = jnp.where(slot < filled[e:e + 1, :], slot + place[e:e + 1, :], -1.0) - lane
        for j in range(half * rows // 128):
            dis[e * cap:(e + 1) * cap, j * 128:(j + 1) * 128] = jnp.where(pos == float(j * 128), 1.0, 0.0).astype(BF16)
    whole = place.astype(jnp.int32)
    keyw[...] = jnp.where(key_val >= 0.0, key_val + (whole & 15).astype(F32), -1.0)

    for cp in sq_cps:
        cp.wait_recv()
    tot = (sqs[0:1, :] + sqr[0, 0:1, :]) + (sqr[1, 0:1, :] + sqr[2, 0:1, :])
    inv = lax.rsqrt(tot / model_width + EPS)
    inv = jnp.broadcast_to(inv, (tok, tok)).T
    inv = jnp.concatenate([inv] * (width // 128), axis=1)
    b = (hf * inv * as_row(pre_ref)).astype(BF16)
    lgs[...] = lax.dot_general(wr[...], b, (((1,), (1,)), ((), ())), preferred_element_type=F32)
    lg_cps = gather_small(lgs, lgr, ls_sem, lr_sem)
    def dispatch(g):
        r = g * rows
        xs[r:r + rows, :] = jnp.dot(sel[r:r + rows, :], b, preferred_element_type=F32).astype(BF16)

    dispatch(0)
    mix[...] = jnp.zeros_like(mix)

    pos_cp = pltpu.make_async_copy(posv, poss, pos_sem)

    def window_starts():
        ids = jnp.concatenate([ch[...]] * (tok // top_k), axis=0).T
        expert = lax.broadcasted_iota(jnp.int32, (tok, tok), 1)
        at = lax.broadcasted_iota(jnp.int32, (tok, tok), 0)
        num = jnp.zeros((tok, tok), jnp.int32)
        for k in range(top_k):
            num = num + jnp.where(ids[:, k:k + 1] == expert, 1, 0)
        num = jnp.minimum(jnp.sum(num, axis=0, keepdims=True), cap)
        num = jnp.broadcast_to(num, (tok, tok)).T
        off = jnp.sum(jnp.where(at < expert, num, 0), axis=0, keepdims=True)
        base = jnp.maximum(expert[0:1, :] // GE - half, 0) * rows - off
        base = jnp.broadcast_to(base, (tok, tok)).T
        pos = off + jnp.max(jnp.where(at <= expert, base, -slots), axis=0, keepdims=True)
        pos = jnp.minimum(pos, half * rows)
        posv[...] = jnp.broadcast_to(pos >> 4, (8, tok))
        pos_cp.start()

    def softmax():
        lg = (lgs[...] + lgr[0]) + (lgr[1] + lgr[2])
        lg = lg - jnp.max(lg, axis=0, keepdims=True)
        ex = jnp.exp(lg)
        probs[...] = ex / jnp.sum(ex, axis=0, keepdims=True)

    def windows(g):
        w = lax.broadcasted_iota(jnp.int32, (WIN, tok), 0).astype(F32)
        for e in range(g * GE, (g + 1) * GE):
            hit = keyw[e:e + 1, :] == w
            selw[e * WIN:(e + 1) * WIN, :] = jnp.where(hit, 1.0, 0.0).astype(BF16)
            picked = jnp.sum(jnp.where(hit, probs[e:e + 1, :], 0.0), axis=1, keepdims=True)
            gate[e * WIN:(e + 1) * WIN, :] = jnp.broadcast_to(picked, (WIN, 128))

    def send_z(i):
        return pltpu.make_async_remote_copy(zc.at[i, oc], rza.at[i], as_sem.at[i], ar_sem.at[i],
                                            device_id=mate, device_id_type=MESH)

    def send_s(i):
        return pltpu.make_async_remote_copy(zc.at[i, c, ox], rzb.at[i], bs_sem.at[i], br_sem.at[i],
                                            device_id=across, device_id_type=MESH)

    def g_copy(i, a, b, send, recv, peer):
        row = (i % half) * rows + (2 * a + b) * quarter
        ref = gbuf.at[i // half, pl.ds(pl.multiple_of(row, quarter), quarter), :]
        return pltpu.make_async_remote_copy(ref, ref, send.at[i], recv.at[i], device_id=peer, device_id_type=MESH)

    def send_g(i):
        return (g_copy(i, c, x, gcs_sem, gcr_sem, mate), g_copy(i, c, x, gxs_sem, gxr_sem, across))

    def recv_mate(i):
        return g_copy(i, oc, x, gcs_sem, gcr_sem, mate)

    def recv_across(i):
        return g_copy(i, c, ox, gxs_sem, gxr_sem, across)

    def forward_g(i):
        return g_copy(i, c, ox, gfs_sem, gfr_sem, mate)

    def recv_forward(i):
        return g_copy(i, oc, ox, gfs_sem, gfr_sem, mate)

    def stage_a(p, g):
        s = (p * groups + g) % NR
        for k in range(GE):
            r = (g * GE + k) * cap
            xe = xs[r:r + cap, :]
            zs[r:r + cap, 0:fw] = jnp.dot(xe, wg[s, k], preferred_element_type=F32).astype(BF16)
            zs[r:r + cap, fw:2 * fw] = jnp.dot(xe, wu[s, k], preferred_element_type=F32).astype(BF16)

    def compact(i):
        k = i % half
        lo, hi = k * rows, (k + half + 1) * rows
        z = lax.dot_general(dis[lo:hi, k * rows:(k + 1) * rows], zs[lo:hi, :], dn,
                            preferred_element_type=F32).astype(BF16)
        for q in range(4):
            zc[i, q // 2, q % 2] = z[q * quarter:(q + 1) * quarter]
        send_z(i).start()

    def stage_b(i):
        zc[i, c, ox] = (zc[i, c, ox].astype(F32) + rza[i, ox].astype(F32)).astype(BF16)
        send_s(i).start()

    def stage_c(i):
        z = (zc[i, c, x].astype(F32) + rza[i, x].astype(F32) + rzb[i].astype(F32)).astype(BF16).astype(F32)
        prod = jax.nn.gelu(z[:, 0:fw], approximate=True) * z[:, fw:2 * fw]
        row = (i % half) * rows + (2 * c + x) * quarter
        gbuf[i // half, pl.ds(pl.multiple_of(row, quarter), quarter), :] = prod.astype(BF16)
        for cp in send_g(i):
            cp.start()

    def exchange(b_list, c_list, d_list):
        for i in b_list:
            send_z(i).wait_recv()
        for i in c_list:
            send_s(i).wait_recv()
        for i in d_list:
            recv_across(i).wait_recv()
        for i in b_list:
            stage_b(i)
        for i in c_list:
            stage_c(i)
        for i in d_list:
            forward_g(i).start()

    def arrived(i):
        recv_mate(i).wait_recv()
        recv_forward(i).wait_recv()
        p, r = i // half, (i % half) * rows
        act[r // 16:(r + rows) // 16, :, p * fw:(p + 1) * fw] = gbuf[p, r:r + rows, :].reshape(rows // 16, 16, fw)

    def down(g, h):
        cols = slice(h * hw, (h + 1) * hw)
        us = []
        for k in range(GE):
            e = g * GE + k
            at = poss[0, e]
            win = jnp.concatenate([act[at + j] for j in range(WIN // 16)], axis=0)
            y = jnp.dot(win, wd[g, k, :, cols], preferred_element_type=F32)
            gk = gate[e * WIN:(e + 1) * WIN, :]
            gk = jnp.concatenate([gk] * (hw // 128), axis=1)
            us.append(jnp.where(gk > 0.0, y.astype(BF16).astype(F32) * gk, 0.0).astype(BF16))
        u = jnp.concatenate(us, axis=0)
        r = g * GE * WIN
        mix[h] += lax.dot_general(selw[r:r + GE * WIN, :], u, dn, preferred_element_type=F32)

    hw = width // 2
    b_at = {6: (0,), 7: (1,), 8: (2,), 9: (3,), 14: (4,), 15: (5,)}
    c_at = {10: (0,), 11: (1,), 12: (2,), 14: (3,)}
    d_at = {14: (0,), 15: (1,)}
    for t in range(NP * groups):
        p, g = divmod(t, groups)
        for cp in weight_copies(p, g):
            cp.wait()
        if t == 3:
            for cp in lg_cps:
                cp.wait_recv()
        exchange(b_at.get(t, ()), c_at.get(t, ()), d_at.get(t, ()))
        if g > half:
            compact(p * half + g - half - 1)
        elif g == 0 and p > 0:
            compact(p * half - 1)
        stage_a(p, g)
        if p == 0 and g + 1 < groups:
            dispatch(g + 1)
        if t == 2:
            window_starts()
        if t == 3:
            softmax()
        if 4 <= t < 4 + groups:
            windows(t - 4)
        if t + NR < NP * groups:
            for cp in weight_copies(*divmod(t + NR, groups)):
                cp.start()
        elif t + NR < NP * groups + 2:
            down_copy(t + NR - NP * groups + 2).start()
        else:
            for h in range(4, groups):
                down_copy(h).start()

    exchange((6,), (), (2,))
    compact(7)
    pos_cp.wait()
    exchange((), (4,), (3,))
    exchange((7,), (), ())
    for i in range(half):
        arrived(i)
    exchange((), (5,), ())
    exchange((), (6,), (4,))
    exchange((), (7,), ())
    exchange((), (), (5,))
    arrived(4)
    down_copy(0).wait()
    down(0, 0)
    exchange((), (), (6,))
    down(0, 1)
    arrived(5)
    down_copy(1).wait()
    down(1, 0)
    exchange((), (), (7,))
    down(1, 1)
    arrived(6)
    down_copy(2).wait()
    down(2, 0)
    down(2, 1)
    for g in range(3, groups):
        down_copy(g).wait()
    arrived(7)
    for h in range(2):
        for g in range(3, groups):
            down(g, h)
        pltpu.make_async_remote_copy(mix.at[h], rmix.at[h], ms_sem.at[h], mr_sem.at[h],
                                     device_id=other, device_id_type=MESH).start()

    for i in range(NP * half):
        send_z(i).wait_send()
        send_s(i).wait_send()
        for cp in send_g(i):
            cp.wait_send()
        forward_g(i).wait_send()
    for cp in sq_cps + lg_cps:
        cp.wait_send()
    ms = []
    for h in range(2):
        pltpu.make_async_remote_copy(mix.at[h], rmix.at[h], ms_sem.at[h], mr_sem.at[h],
                                     device_id=other, device_id_type=MESH).wait()
        ms.append(mix[h] + rmix[h])
    m = jnp.concatenate(ms, axis=1)
    sqs2[...] = row_sums(m * m)
    cps = gather_small(sqs2, sqr2, ps_sem, pr_sem)
    for cp in cps:
        cp.wait()
    tot = (sqs2[0:1, :] + sqr2[0, 0:1, :]) + (sqr2[1, 0:1, :] + sqr2[2, 0:1, :])
    inv = lax.rsqrt(tot / model_width + EPS)
    inv = jnp.broadcast_to(inv, (tok, tok)).T
    inv = jnp.concatenate([inv] * (width // 128), axis=1)
    out_ref[...] = (hid[...].astype(F32) + m * inv * as_row(post_ref)).astype(BF16)


def solution(mesh):
    emb_size = mesh.shape["emb"]

    def local_block(hidden, norm_pre, norm_post, w_router, w_gate, w_up, w_down, choice):
        tok, width = hidden.shape
        experts, _, wid = w_gate.shape
        top_k = choice.shape[1]
        cap = 2 * tok * top_k // experts
        groups = experts // GE
        nblk = NP * groups // 2
        slots, quarter, fw = experts * cap, GE * cap // 4, wid // NP
        dma = pltpu.SemaphoreType.DMA
        vmem = pltpu.VMEM
        assert emb_size == 4 and wid == width and slots == 2 * tok * top_k and WIN == cap + 16
        hbm = pl.BlockSpec(memory_space=pl.ANY)
        vm = pl.BlockSpec(memory_space=pltpu.VMEM)
        return pl.pallas_call(
            functools.partial(kernel, tok, wid, experts, cap, width, top_k, width * emb_size),
            out_shape=jax.ShapeDtypeStruct((tok, width), BF16),
            in_specs=[hbm, vm, vm, hbm, hbm, hbm, hbm, hbm],
            out_specs=vm,
            scratch_shapes=[
                vmem((tok, width), BF16), vmem((experts, width), BF16), vmem((top_k, tok), jnp.int32),
                vmem((NR, GE, width, fw), BF16), vmem((NR, GE, width, fw), BF16), vmem((groups, GE, wid, width), BF16),
                vmem((slots, width), BF16), vmem((slots, tok), BF16), vmem((slots, slots // 2), BF16),
                vmem((experts, tok), F32), vmem((experts, tok), F32), vmem((experts * WIN, tok), BF16), vmem((experts * WIN, 128), F32),
                vmem((8, tok), jnp.int32), pltpu.SMEM((8, tok), jnp.int32),
                vmem((slots, 2 * fw), BF16), vmem((nblk, 2, 2, quarter, 2 * fw), BF16), vmem((nblk, 2, quarter, 2 * fw), BF16),
                vmem((nblk, quarter, 2 * fw), BF16),
                vmem((NP, slots // 2, fw), BF16), vmem(((slots // 2 + WIN) // 16, 16, wid), BF16),
                vmem((2, tok, width // 2), F32), vmem((2, tok, width // 2), F32),
                vmem((8, tok), F32), vmem((3, 8, tok), F32),
                vmem((experts, tok), F32), vmem((3, experts, tok), F32),
                vmem((8, tok), F32), vmem((3, 8, tok), F32),
                dma((3,)), dma, dma((NR,)), dma((NR,)), dma((groups,)),
            ] + [dma((nblk,))] * 10 + [dma((3,))] * 6 + [dma((2,))] * 2,
            compiler_params=pltpu.CompilerParams(
                collective_id=0, has_side_effects=True, vmem_limit_bytes=67043328),
        )(hidden, norm_pre.reshape(width // 128, 128), norm_post.reshape(width // 128, 128), w_router.T, w_gate, w_up, w_down, choice.T)

    in_specs = (P("dp", "emb"), P("emb"), P("emb"), P("emb", None), P(None, "emb", "ffn"), P(None, "emb", "ffn"), P(None, "ffn", "emb"), P("dp", None))
    return jax.shard_map(local_block, mesh=mesh, in_specs=in_specs, out_specs=P("dp", "emb"), check_vma=False)
```

```python
import functools

import jax
import jax.numpy as jnp
from jax import lax
from jax.experimental import pallas as pl
from jax.experimental.pallas import tpu as pltpu
from jax.sharding import PartitionSpec as P

EPS = 1e-5
MESH = pl.DeviceIdType.MESH
F32 = jnp.float32
BF16 = jnp.bfloat16

GE = 16
GD = 8
NP = 4
NR = 3
WIN = 48


def kernel(tok, wid, experts, cap, width, top_k, model_width,
           hid_hbm, pre_ref, post_ref, wr_hbm, wg_hbm, wu_hbm, wd_hbm, ch_hbm, out_ref,
           hid, wr, ch, wgu, wd, xs, sel, dis, keyw, probs, selw, gate, posv, poss, zs, zc, rza, rzb, gbuf, act, mix, rmix,
           sqs, sqr, lgs, lgr, sqs2, sqr2,
           small_sem, pos_sem, wg_sem, wu_sem, wd_sem,
           as_sem, ar_sem, bs_sem, br_sem, gcs_sem, gcr_sem, gxs_sem, gxr_sem, gfs_sem, gfr_sem,
           ss_sem, sr_sem, ls_sem, lr_sem, ps_sem, pr_sem, ms_sem, mr_sem):
    groups = experts // GE
    half = groups // 2
    rows = GE * cap
    downs = experts // GD
    slots = experts * cap
    quarter = rows // 4
    fw = wid // NP
    emb = lax.axis_index("emb")
    ffn = lax.axis_index("ffn")
    x, c = emb // 2, emb % 2
    ox, oc = 1 - x, 1 - c
    mate = {"emb": x * 2 + oc}
    across = {"emb": ox * 2 + c}
    diag = {"emb": ox * 2 + oc}
    other = {"ffn": 1 - ffn}
    peers = (mate, across, diag)

    def weight_copies(p, g):
        e = pl.ds(g * GE, GE)
        col = pl.ds(p * fw, fw)
        s = (p * groups + g) % NR
        return (pltpu.make_async_copy(wg_hbm.at[e, :, col], wgu.at[s, :, :, 0:fw], wg_sem.at[s]),
                pltpu.make_async_copy(wu_hbm.at[e, :, col], wgu.at[s, :, :, fw:2 * fw], wu_sem.at[s]))

    def down_copy(g):
        return pltpu.make_async_copy(wd_hbm.at[pl.ds(g * GD, GD)], wd.at[g], wd_sem.at[g])

    small = (pltpu.make_async_copy(hid_hbm, hid, small_sem.at[0]),
             pltpu.make_async_copy(ch_hbm, ch, small_sem.at[1]),
             pltpu.make_async_copy(wr_hbm, wr, small_sem.at[2]))
    for cp in small:
        cp.start()
    barrier = pltpu.get_barrier_semaphore()
    for peer in peers + (other,):
        pl.semaphore_signal(barrier, inc=1, device_id=peer, device_id_type=MESH)

    def gather_small(src, dst, send, recv):
        cps = [pltpu.make_async_remote_copy(src, dst.at[j], send.at[j], recv.at[j], device_id=peer, device_id_type=MESH)
               for j, peer in enumerate(peers)]
        for cp in cps:
            cp.start()
        return cps

    def row_sums(sq):
        part = sq[:, 0:128]
        for j in range(1, width // 128):
            part = part + sq[:, j * 128:(j + 1) * 128]
        t = jnp.sum(part.T, axis=0, keepdims=True)
        return jnp.broadcast_to(t, (8, tok))

    def as_row(ref):
        v = ref[...].astype(F32)
        return jnp.concatenate([v[j:j + 1, :] for j in range(width // 128)], axis=1)

    for cp in small:
        cp.wait()
    for g in range(NR):
        for cp in weight_copies(0, g):
            cp.start()
    down_copy(0).start()
    down_copy(1).start()
    hf = hid[...].astype(F32)
    sqs[...] = row_sums(hf * hf)
    pl.semaphore_wait(barrier, 4)
    sq_cps = gather_small(sqs, sqr, ss_sem, sr_sem)

    expert_id = lax.broadcasted_iota(jnp.int32, (experts, tok), 0)
    chv = ch[...]
    hot = jnp.zeros((experts, tok), F32)
    for k in range(top_k):
        hot = hot + jnp.where(chv[k:k + 1, :] == expert_id, 1.0, 0.0)
    t0 = lax.broadcasted_iota(jnp.int32, (tok, tok), 0)
    t1 = lax.broadcasted_iota(jnp.int32, (tok, tok), 1)
    upper = jnp.where(t0 < t1, 1.0, 0.0).astype(BF16)
    before = jnp.dot(hot.astype(BF16), upper, preferred_element_type=F32)
    key_val = jnp.where((hot > 0.5) & (before < cap - 0.5), before, -1.0)
    dn = (((0,), (0,)), ((), ()))
    slot = lax.broadcasted_iota(jnp.int32, (cap, tok), 0).astype(F32)
    for e in range(experts):
        sel[e * cap:(e + 1) * cap, :] = jnp.where(key_val[e:e + 1, :] == slot, 1.0, 0.0).astype(BF16)

    filled = jnp.broadcast_to(jnp.minimum(jnp.sum(hot, axis=1, keepdims=True), float(cap)), (experts, 128))
    e0 = lax.broadcasted_iota(jnp.int32, (experts, experts), 0)
    e1 = lax.broadcasted_iota(jnp.int32, (experts, experts), 1)
    lower = jnp.where(e1 < e0, 1.0, 0.0).astype(BF16)
    start = jnp.dot(lower, filled.astype(BF16), preferred_element_type=F32)
    lane = lax.broadcasted_iota(jnp.int32, (cap, 128), 1).astype(F32)
    shift = jnp.zeros((1, 128), F32)
    place = []
    for g in range(groups):
        base = float(max(0, rows * (g - half)))
        shift = jnp.maximum(shift, base - start[g * GE:g * GE + 1, :])
        place.append(start[g * GE:(g + 1) * GE, :] + shift)
    place = jnp.concatenate(place, axis=0)
    for e in range(experts):
        pos = jnp.where(slot < filled[e:e + 1, :], slot + place[e:e + 1, :], -1.0) - lane
        for j in range(half * rows // 128):
            dis[e * cap:(e + 1) * cap, j * 128:(j + 1) * 128] = jnp.where(pos == float(j * 128), 1.0, 0.0).astype(BF16)
    whole = place.astype(jnp.int32)
    keyw[...] = jnp.where(key_val >= 0.0, key_val + (whole & 15).astype(F32), -1.0)

    for cp in sq_cps:
        cp.wait_recv()
    tot = (sqs[0:1, :] + sqr[0, 0:1, :]) + (sqr[1, 0:1, :] + sqr[2, 0:1, :])
    inv = lax.rsqrt(tot / model_width + EPS)
    inv = jnp.broadcast_to(inv, (tok, tok)).T
    inv = jnp.concatenate([inv] * (width // 128), axis=1)
    b = (hf * inv * as_row(pre_ref)).astype(BF16)
    lgs[...] = lax.dot_general(wr[...], b, (((1,), (1,)), ((), ())), preferred_element_type=F32)
    lg_cps = gather_small(lgs, lgr, ls_sem, lr_sem)
    def dispatch(g):
        for r in range(g * rows, (g + 1) * rows, 256):
            xs[r:r + 256, :] = jnp.dot(sel[r:r + 256, :], b, preferred_element_type=F32).astype(BF16)

    dispatch(0)
    mix[...] = jnp.zeros_like(mix)

    pos_cp = pltpu.make_async_copy(posv, poss, pos_sem)

    def window_starts():
        ids = jnp.concatenate([ch[...]] * (tok // top_k), axis=0).T
        expert = lax.broadcasted_iota(jnp.int32, (tok, tok), 1)
        at = lax.broadcasted_iota(jnp.int32, (tok, tok), 0)
        num = jnp.zeros((tok, tok), jnp.int32)
        for k in range(top_k):
            num = num + jnp.where(ids[:, k:k + 1] == expert, 1, 0)
        num = jnp.minimum(jnp.sum(num, axis=0, keepdims=True), cap)
        num = jnp.broadcast_to(num, (tok, tok)).T
        off = jnp.sum(jnp.where(at < expert, num, 0), axis=0, keepdims=True)
        base = jnp.maximum(expert[0:1, :] // GE - half, 0) * rows - off
        base = jnp.broadcast_to(base, (tok, tok)).T
        pos = off + jnp.max(jnp.where(at <= expert, base, -slots), axis=0, keepdims=True)
        pos = jnp.minimum(pos, half * rows)
        posv[...] = jnp.broadcast_to(pos >> 4, (8, tok))
        pos_cp.start()

    def softmax():
        lg = (lgs[...] + lgr[0]) + (lgr[1] + lgr[2])
        lg = lg - jnp.max(lg, axis=0, keepdims=True)
        ex = jnp.exp(lg)
        probs[...] = ex / jnp.sum(ex, axis=0, keepdims=True)

    def windows(g):
        w = lax.broadcasted_iota(jnp.int32, (WIN, tok), 0).astype(F32)
        for e in range(g * GD, (g + 1) * GD):
            hit = keyw[e:e + 1, :] == w
            selw[e * WIN:(e + 1) * WIN, :] = jnp.where(hit, 1.0, 0.0).astype(BF16)
            picked = jnp.sum(jnp.where(hit, probs[e:e + 1, :], 0.0), axis=1, keepdims=True)
            gate[e * WIN:(e + 1) * WIN, :] = jnp.broadcast_to(picked, (WIN, 128))

    def send_z(i):
        return pltpu.make_async_remote_copy(zc.at[i, oc], rza.at[i], as_sem.at[i], ar_sem.at[i],
                                            device_id=mate, device_id_type=MESH)

    def send_s(i):
        return pltpu.make_async_remote_copy(zc.at[i, c, ox], rzb.at[i], bs_sem.at[i], br_sem.at[i],
                                            device_id=across, device_id_type=MESH)

    def g_copy(i, a, b, send, recv, peer):
        row = (i % half) * rows + (2 * a + b) * quarter
        ref = gbuf.at[i // half, pl.ds(pl.multiple_of(row, quarter), quarter), :]
        return pltpu.make_async_remote_copy(ref, ref, send.at[i], recv.at[i], device_id=peer, device_id_type=MESH)

    def send_g(i):
        return (g_copy(i, c, x, gcs_sem, gcr_sem, mate), g_copy(i, c, x, gxs_sem, gxr_sem, across))

    def recv_mate(i):
        return g_copy(i, oc, x, gcs_sem, gcr_sem, mate)

    def recv_across(i):
        return g_copy(i, c, ox, gxs_sem, gxr_sem, across)

    def forward_g(i):
        return g_copy(i, c, ox, gfs_sem, gfr_sem, mate)

    def recv_forward(i):
        return g_copy(i, oc, ox, gfs_sem, gfr_sem, mate)

    def stage_a(p, g):
        s = (p * groups + g) % NR
        for k in range(GE):
            r = (g * GE + k) * cap
            xe = xs[r:r + cap, :]
            zs[r:r + cap, :] = jnp.dot(xe, wgu[s, k], preferred_element_type=F32).astype(BF16)

    def compact(i):
        k = i % half
        lo, hi = k * rows, (k + half + 1) * rows
        z = lax.dot_general(dis[lo:hi, k * rows:(k + 1) * rows], zs[lo:hi, :], dn,
                            preferred_element_type=F32).astype(BF16)
        for q in range(4):
            zc[i, q // 2, q % 2] = z[q * quarter:(q + 1) * quarter]
        send_z(i).start()

    def stage_b(i):
        zc[i, c, ox] = (zc[i, c, ox].astype(F32) + rza[i, ox].astype(F32)).astype(BF16)
        send_s(i).start()

    def stage_c(i):
        z = (zc[i, c, x].astype(F32) + rza[i, x].astype(F32) + rzb[i].astype(F32)).astype(BF16).astype(F32)
        prod = jax.nn.gelu(z[:, 0:fw], approximate=True) * z[:, fw:2 * fw]
        row = (i % half) * rows + (2 * c + x) * quarter
        gbuf[i // half, pl.ds(pl.multiple_of(row, quarter), quarter), :] = prod.astype(BF16)
        for cp in send_g(i):
            cp.start()

    def exchange(b_list, c_list, d_list):
        for i in b_list:
            send_z(i).wait_recv()
        for i in c_list:
            send_s(i).wait_recv()
        for i in d_list:
            recv_across(i).wait_recv()
        for i in b_list:
            stage_b(i)
        for i in c_list:
            stage_c(i)
        for i in d_list:
            forward_g(i).start()

    def arrived(i):
        recv_mate(i).wait_recv()
        recv_forward(i).wait_recv()
        p, r = i // half, (i % half) * rows
        act[r // 16:(r + rows) // 16, :, p * fw:(p + 1) * fw] = gbuf[p, r:r + rows, :].reshape(rows // 16, 16, fw)

    def down(g, h):
        cols = slice(h * hw, (h + 1) * hw)
        us = []
        for k in range(GD):
            e = g * GD + k
            at = poss[0, e]
            win = jnp.concatenate([act[at + j] for j in range(WIN // 16)], axis=0)
            y = jnp.dot(win, wd[g, k, :, cols], preferred_element_type=F32)
            gk = gate[e * WIN:(e + 1) * WIN, :]
            gk = jnp.concatenate([gk] * (hw // 128), axis=1)
            us.append(jnp.where(gk > 0.0, y.astype(BF16).astype(F32) * gk, 0.0).astype(BF16))
        u = jnp.concatenate(us, axis=0)
        r = g * GD * WIN
        mix[h] += lax.dot_general(selw[r:r + GD * WIN, :], u, dn, preferred_element_type=F32)

    hw = width // 2
    b_at = {4: (0,), 5: (1,), 8: (2,), 9: (3,), 12: (4,), 13: (5,)}
    c_at = {7: (0,), 8: (1,), 11: (2,), 12: (3,), 15: (4,)}
    d_at = {10: (0,), 11: (1,), 14: (2,), 15: (3,)}
    for t in range(NP * groups):
        p, g = divmod(t, groups)
        for cp in weight_copies(p, g):
            cp.wait()
        if t == 3:
            for cp in lg_cps:
                cp.wait_recv()
        exchange(b_at.get(t, ()), c_at.get(t, ()), d_at.get(t, ()))
        if g > half:
            compact(p * half + g - half - 1)
        elif g == 0 and p > 0:
            compact(p * half - 1)
        stage_a(p, g)
        if p == 0 and g + 1 < groups:
            dispatch(g + 1)
        if t == 2:
            window_starts()
        if t == 3:
            softmax()
        if 4 <= t < 4 + downs:
            windows(t - 4)
        if t + NR < NP * groups:
            for cp in weight_copies(*divmod(t + NR, groups)):
                cp.start()
        else:
            n = t + NR - NP * groups
            for h in range(2 + 2 * n, 4 + 2 * n):
                down_copy(h).start()

    exchange((6,), (), ())
    compact(7)
    exchange((), (5,), (4,))
    exchange((7,), (), ())
    pos_cp.wait()
    for i in range(4):
        arrived(i)
    for g in range(downs):
        down_copy(g).wait()
    exchange((), (6,), (5,))
    arrived(4)
    exchange((), (7,), ())
    arrived(5)
    exchange((), (), (6,))
    arrived(6)
    down(0, 0)
    exchange((), (), (7,))
    down(0, 1)
    down(1, 0)
    down(1, 1)
    arrived(7)
    for h in range(2):
        for g in range(2, downs):
            down(g, h)
        pltpu.make_async_remote_copy(mix.at[h], rmix.at[h], ms_sem.at[h], mr_sem.at[h],
                                     device_id=other, device_id_type=MESH).start()

    for i in range(NP * half):
        send_z(i).wait_send()
        send_s(i).wait_send()
        for cp in send_g(i):
            cp.wait_send()
        forward_g(i).wait_send()
    for cp in sq_cps + lg_cps:
        cp.wait_send()
    ms = []
    for h in range(2):
        pltpu.make_async_remote_copy(mix.at[h], rmix.at[h], ms_sem.at[h], mr_sem.at[h],
                                     device_id=other, device_id_type=MESH).wait()
        ms.append(mix[h] + rmix[h])
    m = jnp.concatenate(ms, axis=1)
    sqs2[...] = row_sums(m * m)
    cps = gather_small(sqs2, sqr2, ps_sem, pr_sem)
    for cp in cps:
        cp.wait()
    tot = (sqs2[0:1, :] + sqr2[0, 0:1, :]) + (sqr2[1, 0:1, :] + sqr2[2, 0:1, :])
    inv = lax.rsqrt(tot / model_width + EPS)
    inv = jnp.broadcast_to(inv, (tok, tok)).T
    inv = jnp.concatenate([inv] * (width // 128), axis=1)
    out_ref[...] = (hid[...].astype(F32) + m * inv * as_row(post_ref)).astype(BF16)


def solution(mesh):
    emb_size = mesh.shape["emb"]

    def local_block(hidden, norm_pre, norm_post, w_router, w_gate, w_up, w_down, choice):
        tok, width = hidden.shape
        experts, _, wid = w_gate.shape
        top_k = choice.shape[1]
        cap = 2 * tok * top_k // experts
        groups = experts // GE
        nblk = NP * groups // 2
        slots, quarter, fw = experts * cap, GE * cap // 4, wid // NP
        dma = pltpu.SemaphoreType.DMA
        vmem = pltpu.VMEM
        assert emb_size == 4 and wid == width and slots == 2 * tok * top_k and WIN == cap + 16
        hbm = pl.BlockSpec(memory_space=pl.ANY)
        vm = pl.BlockSpec(memory_space=pltpu.VMEM)
        return pl.pallas_call(
            functools.partial(kernel, tok, wid, experts, cap, width, top_k, width * emb_size),
            out_shape=jax.ShapeDtypeStruct((tok, width), BF16),
            in_specs=[hbm, vm, vm, hbm, hbm, hbm, hbm, hbm],
            out_specs=vm,
            scratch_shapes=[
                vmem((tok, width), BF16), vmem((experts, width), BF16), vmem((top_k, tok), jnp.int32),
                vmem((NR, GE, width, 2 * fw), BF16), vmem((experts // GD, GD, wid, width), BF16),
                vmem((slots, width), BF16), vmem((slots, tok), BF16), vmem((slots, slots // 2), BF16),
                vmem((experts, tok), F32), vmem((experts, tok), F32), vmem((experts * WIN, tok), BF16), vmem((experts * WIN, 128), F32),
                vmem((8, tok), jnp.int32), pltpu.SMEM((8, tok), jnp.int32),
                vmem((slots, 2 * fw), BF16), vmem((nblk, 2, 2, quarter, 2 * fw), BF16), vmem((nblk, 2, quarter, 2 * fw), BF16),
                vmem((nblk, quarter, 2 * fw), BF16),
                vmem((NP, slots // 2, fw), BF16), vmem(((slots // 2 + WIN) // 16, 16, wid), BF16),
                vmem((2, tok, width // 2), F32), vmem((2, tok, width // 2), F32),
                vmem((8, tok), F32), vmem((3, 8, tok), F32),
                vmem((experts, tok), F32), vmem((3, experts, tok), F32),
                vmem((8, tok), F32), vmem((3, 8, tok), F32),
                dma((3,)), dma, dma((NR,)), dma((NR,)), dma((experts // GD,)),
            ] + [dma((nblk,))] * 10 + [dma((3,))] * 6 + [dma((2,))] * 2,
            compiler_params=pltpu.CompilerParams(
                collective_id=0, has_side_effects=True, vmem_limit_bytes=67043328),
        )(hidden, norm_pre.reshape(width // 128, 128), norm_post.reshape(width // 128, 128), w_router.T, w_gate, w_up, w_down, choice.T)

    in_specs = (P("dp", "emb"), P("emb"), P("emb"), P("emb", None), P(None, "emb", "ffn"), P(None, "emb", "ffn"), P(None, "ffn", "emb"), P("dp", None))
    return jax.shard_map(local_block, mesh=mesh, in_specs=in_specs, out_specs=P("dp", "emb"), check_vma=False)
```

```python
import functools

import jax
import jax.numpy as jnp
from jax import lax
from jax.experimental import pallas as pl
from jax.experimental.pallas import tpu as pltpu
from jax.sharding import PartitionSpec as P

EPS = 1e-5
MESH = pl.DeviceIdType.MESH
F32 = jnp.float32
BF16 = jnp.bfloat16

GE = 8
NP = 2
NR = 3
WIN = 48


def kernel(tok, wid, experts, cap, width, top_k, model_width,
           hid_hbm, pre_ref, post_ref, wr_hbm, wg_hbm, wu_hbm, wd_hbm, ch_hbm, out_ref,
           hid, wr, ch, wg, wu, wd, xs, sel, dis, keyw, probs, selw, gate, posv, poss, zs, zc, rza, rzb, gbuf, act, mix, rmix,
           sqs, sqr, lgs, lgr, sqs2, sqr2,
           small_sem, pos_sem, wg_sem, wu_sem, wd_sem,
           as_sem, ar_sem, bs_sem, br_sem, gcs_sem, gcr_sem, gxs_sem, gxr_sem, gfs_sem, gfr_sem,
           ss_sem, sr_sem, ls_sem, lr_sem, ps_sem, pr_sem, ms_sem, mr_sem):
    groups = experts // GE
    half = groups // 2
    rows = GE * cap
    slots = experts * cap
    quarter = rows // 4
    fw = wid // NP
    emb = lax.axis_index("emb")
    ffn = lax.axis_index("ffn")
    x, c = emb // 2, emb % 2
    ox, oc = 1 - x, 1 - c
    mate = {"emb": x * 2 + oc}
    across = {"emb": ox * 2 + c}
    diag = {"emb": ox * 2 + oc}
    other = {"ffn": 1 - ffn}
    peers = (mate, across, diag)

    def weight_copies(p, g):
        e = pl.ds(g * GE, GE)
        col = pl.ds(p * fw, fw)
        s = (p * groups + g) % NR
        return (pltpu.make_async_copy(wg_hbm.at[e, :, col], wg.at[s], wg_sem.at[s]),
                pltpu.make_async_copy(wu_hbm.at[e, :, col], wu.at[s], wu_sem.at[s]))

    def down_copy(g):
        return pltpu.make_async_copy(wd_hbm.at[pl.ds(g * GE, GE)], wd.at[g], wd_sem.at[g])

    small = (pltpu.make_async_copy(hid_hbm, hid, small_sem.at[0]),
             pltpu.make_async_copy(ch_hbm, ch, small_sem.at[1]),
             pltpu.make_async_copy(wr_hbm, wr, small_sem.at[2]))
    for cp in small:
        cp.start()
    barrier = pltpu.get_barrier_semaphore()
    for peer in peers + (other,):
        pl.semaphore_signal(barrier, inc=1, device_id=peer, device_id_type=MESH)

    def gather_small(src, dst, send, recv):
        cps = [pltpu.make_async_remote_copy(src, dst.at[j], send.at[j], recv.at[j], device_id=peer, device_id_type=MESH)
               for j, peer in enumerate(peers)]
        for cp in cps:
            cp.start()
        return cps

    def row_sums(sq):
        part = sq[:, 0:128]
        for j in range(1, width // 128):
            part = part + sq[:, j * 128:(j + 1) * 128]
        t = jnp.sum(part.T, axis=0, keepdims=True)
        return jnp.broadcast_to(t, (8, tok))

    def as_row(ref):
        v = ref[...].astype(F32)
        return jnp.concatenate([v[j:j + 1, :] for j in range(width // 128)], axis=1)

    for cp in small:
        cp.wait()
    for g in range(NR):
        for cp in weight_copies(0, g):
            cp.start()
    down_copy(0).start()
    down_copy(1).start()
    hf = hid[...].astype(F32)
    sqs[...] = row_sums(hf * hf)
    pl.semaphore_wait(barrier, 4)
    sq_cps = gather_small(sqs, sqr, ss_sem, sr_sem)

    expert_id = lax.broadcasted_iota(jnp.int32, (experts, tok), 0)
    chv = ch[...]
    hot = jnp.zeros((experts, tok), F32)
    for k in range(top_k):
        hot = hot + jnp.where(chv[k:k + 1, :] == expert_id, 1.0, 0.0)
    t0 = lax.broadcasted_iota(jnp.int32, (tok, tok), 0)
    t1 = lax.broadcasted_iota(jnp.int32, (tok, tok), 1)
    upper = jnp.where(t0 < t1, 1.0, 0.0).astype(BF16)
    before = jnp.dot(hot.astype(BF16), upper, preferred_element_type=F32)
    key_val = jnp.where((hot > 0.5) & (before < cap - 0.5), before, -1.0)
    dn = (((0,), (0,)), ((), ()))
    slot = lax.broadcasted_iota(jnp.int32, (cap, tok), 0).astype(F32)
    for e in range(experts):
        sel[e * cap:(e + 1) * cap, :] = jnp.where(key_val[e:e + 1, :] == slot, 1.0, 0.0).astype(BF16)

    filled = jnp.broadcast_to(jnp.minimum(jnp.sum(hot, axis=1, keepdims=True), float(cap)), (experts, 128))
    e0 = lax.broadcasted_iota(jnp.int32, (experts, experts), 0)
    e1 = lax.broadcasted_iota(jnp.int32, (experts, experts), 1)
    lower = jnp.where(e1 < e0, 1.0, 0.0).astype(BF16)
    start = jnp.dot(lower, filled.astype(BF16), preferred_element_type=F32)
    lane = lax.broadcasted_iota(jnp.int32, (cap, 128), 1).astype(F32)
    shift = jnp.zeros((1, 128), F32)
    place = []
    for g in range(groups):
        base = float(max(0, rows * (g - half)))
        shift = jnp.maximum(shift, base - start[g * GE:g * GE + 1, :])
        place.append(start[g * GE:(g + 1) * GE, :] + shift)
    place = jnp.concatenate(place, axis=0)
    for e in range(experts):
        pos = jnp.where(slot < filled[e:e + 1, :], slot + place[e:e + 1, :], -1.0) - lane
        for j in range(half * rows // 128):
            dis[e * cap:(e + 1) * cap, j * 128:(j + 1) * 128] = jnp.where(pos == float(j * 128), 1.0, 0.0).astype(BF16)
    whole = place.astype(jnp.int32)
    keyw[...] = jnp.where(key_val >= 0.0, key_val + (whole & 15).astype(F32), -1.0)

    for cp in sq_cps:
        cp.wait_recv()
    tot = (sqs[0:1, :] + sqr[0, 0:1, :]) + (sqr[1, 0:1, :] + sqr[2, 0:1, :])
    inv = lax.rsqrt(tot / model_width + EPS)
    inv = jnp.broadcast_to(inv, (tok, tok)).T
    inv = jnp.concatenate([inv] * (width // 128), axis=1)
    b = (hf * inv * as_row(pre_ref)).astype(BF16)
    lgs[...] = lax.dot_general(wr[...], b, (((1,), (1,)), ((), ())), preferred_element_type=F32)
    lg_cps = gather_small(lgs, lgr, ls_sem, lr_sem)
    def dispatch(g):
        r = g * rows
        xs[r:r + rows, :] = jnp.dot(sel[r:r + rows, :], b, preferred_element_type=F32).astype(BF16)

    dispatch(0)
    mix[...] = jnp.zeros_like(mix)

    pos_cp = pltpu.make_async_copy(posv, poss, pos_sem)

    def window_starts():
        ids = jnp.concatenate([ch[...]] * (tok // top_k), axis=0).T
        expert = lax.broadcasted_iota(jnp.int32, (tok, tok), 1)
        at = lax.broadcasted_iota(jnp.int32, (tok, tok), 0)
        num = jnp.zeros((tok, tok), jnp.int32)
        for k in range(top_k):
            num = num + jnp.where(ids[:, k:k + 1] == expert, 1, 0)
        num = jnp.minimum(jnp.sum(num, axis=0, keepdims=True), cap)
        num = jnp.broadcast_to(num, (tok, tok)).T
        off = jnp.sum(jnp.where(at < expert, num, 0), axis=0, keepdims=True)
        base = jnp.maximum(expert[0:1, :] // GE - half, 0) * rows - off
        base = jnp.broadcast_to(base, (tok, tok)).T
        pos = off + jnp.max(jnp.where(at <= expert, base, -slots), axis=0, keepdims=True)
        pos = jnp.minimum(pos, half * rows)
        posv[...] = jnp.broadcast_to(pos >> 4, (8, tok))
        pos_cp.start()

    def softmax():
        lg = (lgs[...] + lgr[0]) + (lgr[1] + lgr[2])
        lg = lg - jnp.max(lg, axis=0, keepdims=True)
        ex = jnp.exp(lg)
        probs[...] = ex / jnp.sum(ex, axis=0, keepdims=True)

    def windows(g):
        w = lax.broadcasted_iota(jnp.int32, (WIN, tok), 0).astype(F32)
        for e in range(g * GE, (g + 1) * GE):
            hit = keyw[e:e + 1, :] == w
            selw[e * WIN:(e + 1) * WIN, :] = jnp.where(hit, 1.0, 0.0).astype(BF16)
            picked = jnp.sum(jnp.where(hit, probs[e:e + 1, :], 0.0), axis=1, keepdims=True)
            gate[e * WIN:(e + 1) * WIN, :] = jnp.broadcast_to(picked, (WIN, 128))

    def send_z(i):
        return pltpu.make_async_remote_copy(zc.at[i, oc], rza.at[i], as_sem.at[i], ar_sem.at[i],
                                            device_id=mate, device_id_type=MESH)

    def send_s(i):
        return pltpu.make_async_remote_copy(zc.at[i, c, ox], rzb.at[i], bs_sem.at[i], br_sem.at[i],
                                            device_id=across, device_id_type=MESH)

    def g_copy(i, a, b, send, recv, peer):
        row = (i % half) * rows + (2 * a + b) * quarter
        ref = gbuf.at[i // half, pl.ds(pl.multiple_of(row, quarter), quarter), :]
        return pltpu.make_async_remote_copy(ref, ref, send.at[i], recv.at[i], device_id=peer, device_id_type=MESH)

    def send_g(i):
        return (g_copy(i, c, x, gcs_sem, gcr_sem, mate), g_copy(i, c, x, gxs_sem, gxr_sem, across))

    def recv_mate(i):
        return g_copy(i, oc, x, gcs_sem, gcr_sem, mate)

    def recv_across(i):
        return g_copy(i, c, ox, gxs_sem, gxr_sem, across)

    def forward_g(i):
        return g_copy(i, c, ox, gfs_sem, gfr_sem, mate)

    def recv_forward(i):
        return g_copy(i, oc, ox, gfs_sem, gfr_sem, mate)

    def stage_a(p, g):
        s = (p * groups + g) % NR
        for k in range(GE):
            r = (g * GE + k) * cap
            xe = xs[r:r + cap, :]
            zs[r:r + cap, 0:fw] = jnp.dot(xe, wg[s, k], preferred_element_type=F32).astype(BF16)
            zs[r:r + cap, fw:2 * fw] = jnp.dot(xe, wu[s, k], preferred_element_type=F32).astype(BF16)

    def compact(i):
        k = i % half
        lo, hi = k * rows, (k + half + 1) * rows
        z = lax.dot_general(dis[lo:hi, k * rows:(k + 1) * rows], zs[lo:hi, :], dn,
                            preferred_element_type=F32).astype(BF16)
        for q in range(4):
            zc[i, q // 2, q % 2] = z[q * quarter:(q + 1) * quarter]
        send_z(i).start()

    def stage_b(i):
        zc[i, c, ox] = (zc[i, c, ox].astype(F32) + rza[i, ox].astype(F32)).astype(BF16)
        send_s(i).start()

    def stage_c(i):
        z = (zc[i, c, x].astype(F32) + rza[i, x].astype(F32) + rzb[i].astype(F32)).astype(BF16).astype(F32)
        prod = jax.nn.gelu(z[:, 0:fw], approximate=True) * z[:, fw:2 * fw]
        row = (i % half) * rows + (2 * c + x) * quarter
        gbuf[i // half, pl.ds(pl.multiple_of(row, quarter), quarter), :] = prod.astype(BF16)
        for cp in send_g(i):
            cp.start()

    def exchange(b_list, c_list, d_list):
        for i in b_list:
            send_z(i).wait_recv()
        for i in c_list:
            send_s(i).wait_recv()
        for i in d_list:
            recv_across(i).wait_recv()
        for i in b_list:
            stage_b(i)
        for i in c_list:
            stage_c(i)
        for i in d_list:
            forward_g(i).start()

    def arrived(i):
        recv_mate(i).wait_recv()
        recv_forward(i).wait_recv()
        p, r = i // half, (i % half) * rows
        act[r // 16:(r + rows) // 16, :, p * fw:(p + 1) * fw] = gbuf[p, r:r + rows, :].reshape(rows // 16, 16, fw)

    def down(g, h):
        cols = slice(h * hw, (h + 1) * hw)
        us = []
        for k in range(GE):
            e = g * GE + k
            at = poss[0, e]
            win = jnp.concatenate([act[at + j] for j in range(WIN // 16)], axis=0)
            y = jnp.dot(win, wd[g, k, :, cols], preferred_element_type=F32)
            gk = gate[e * WIN:(e + 1) * WIN, :]
            gk = jnp.concatenate([gk] * (hw // 128), axis=1)
            us.append(jnp.where(gk > 0.0, y.astype(BF16).astype(F32) * gk, 0.0).astype(BF16))
        u = jnp.concatenate(us, axis=0)
        r = g * GE * WIN
        mix[h] += lax.dot_general(selw[r:r + GE * WIN, :], u, dn, preferred_element_type=F32)

    hw = width // 2
    b_at = {6: (0,), 7: (1,), 8: (2,), 9: (3,), 14: (4,), 15: (5,)}
    c_at = {10: (0,), 11: (1,), 12: (2,), 14: (3,)}
    d_at = {14: (0,), 15: (1,)}
    for t in range(NP * groups):
        p, g = divmod(t, groups)
        for cp in weight_copies(p, g):
            cp.wait()
        if t == 3:
            for cp in lg_cps:
                cp.wait_recv()
        exchange(b_at.get(t, ()), c_at.get(t, ()), d_at.get(t, ()))
        if g > half:
            compact(p * half + g - half - 1)
        elif g == 0 and p > 0:
            compact(p * half - 1)
        if p == 0 and g + 1 < groups:
            dispatch(g + 1)
        stage_a(p, g)
        if t == 2:
            window_starts()
        if t == 3:
            softmax()
        if 4 <= t < 4 + groups:
            windows(t - 4)
        if t + NR < NP * groups:
            for cp in weight_copies(*divmod(t + NR, groups)):
                cp.start()
        elif t + NR < NP * groups + 2:
            down_copy(t + NR - NP * groups + 2).start()
        else:
            for h in range(4, groups):
                down_copy(h).start()

    exchange((6,), (), (2,))
    compact(7)
    pos_cp.wait()
    exchange((), (4,), (3,))
    exchange((7,), (), ())
    for i in range(half):
        arrived(i)
    exchange((), (5,), ())
    exchange((), (6,), (4,))
    for g in range(3):
        down_copy(g).wait()
    exchange((), (7,), (5,))
    arrived(4)
    down(0, 0)
    down(0, 1)
    exchange((), (), (6,))
    arrived(5)
    down(1, 0)
    down(1, 1)
    exchange((), (), (7,))
    arrived(6)
    down(2, 0)
    down(2, 1)
    for g in range(3, groups):
        down_copy(g).wait()
    arrived(7)
    for h in range(2):
        for g in range(3, groups):
            down(g, h)
        pltpu.make_async_remote_copy(mix.at[h], rmix.at[h], ms_sem.at[h], mr_sem.at[h],
                                     device_id=other, device_id_type=MESH).start()

    for i in range(NP * half):
        send_z(i).wait_send()
        send_s(i).wait_send()
        for cp in send_g(i):
            cp.wait_send()
        forward_g(i).wait_send()
    for cp in sq_cps + lg_cps:
        cp.wait_send()
    ms = []
    for h in range(2):
        pltpu.make_async_remote_copy(mix.at[h], rmix.at[h], ms_sem.at[h], mr_sem.at[h],
                                     device_id=other, device_id_type=MESH).wait()
        ms.append(mix[h] + rmix[h])
    m = jnp.concatenate(ms, axis=1)
    sqs2[...] = row_sums(m * m)
    cps = gather_small(sqs2, sqr2, ps_sem, pr_sem)
    for cp in cps:
        cp.wait()
    tot = (sqs2[0:1, :] + sqr2[0, 0:1, :]) + (sqr2[1, 0:1, :] + sqr2[2, 0:1, :])
    inv = lax.rsqrt(tot / model_width + EPS)
    inv = jnp.broadcast_to(inv, (tok, tok)).T
    inv = jnp.concatenate([inv] * (width // 128), axis=1)
    out_ref[...] = (hid[...].astype(F32) + m * inv * as_row(post_ref)).astype(BF16)


def solution(mesh):
    emb_size = mesh.shape["emb"]

    def local_block(hidden, norm_pre, norm_post, w_router, w_gate, w_up, w_down, choice):
        tok, width = hidden.shape
        experts, _, wid = w_gate.shape
        top_k = choice.shape[1]
        cap = 2 * tok * top_k // experts
        groups = experts // GE
        nblk = NP * groups // 2
        slots, quarter, fw = experts * cap, GE * cap // 4, wid // NP
        dma = pltpu.SemaphoreType.DMA
        vmem = pltpu.VMEM
        assert emb_size == 4 and wid == width and slots == 2 * tok * top_k and WIN == cap + 16
        hbm = pl.BlockSpec(memory_space=pl.ANY)
        vm = pl.BlockSpec(memory_space=pltpu.VMEM)
        return pl.pallas_call(
            functools.partial(kernel, tok, wid, experts, cap, width, top_k, width * emb_size),
            out_shape=pltpu.VMEM((tok, width), BF16),
            in_specs=[hbm, vm, vm, hbm, hbm, hbm, hbm, hbm],
            out_specs=vm,
            scratch_shapes=[
                vmem((tok, width), BF16), vmem((experts, width), BF16), vmem((top_k, tok), jnp.int32),
                vmem((NR, GE, width, fw), BF16), vmem((NR, GE, width, fw), BF16), vmem((groups, GE, wid, width), BF16),
                vmem((slots, width), BF16), vmem((slots, tok), BF16), vmem((slots, slots // 2), BF16),
                vmem((experts, tok), F32), vmem((experts, tok), F32), vmem((experts * WIN, tok), BF16), vmem((experts * WIN, 128), F32),
                vmem((8, tok), jnp.int32), pltpu.SMEM((8, tok), jnp.int32),
                vmem((slots, 2 * fw), BF16), vmem((nblk, 2, 2, quarter, 2 * fw), BF16), vmem((nblk, 2, quarter, 2 * fw), BF16),
                vmem((nblk, quarter, 2 * fw), BF16),
                vmem((NP, slots // 2, fw), BF16), vmem(((slots // 2 + WIN) // 16, 16, wid), BF16),
                vmem((2, tok, width // 2), F32), vmem((2, tok, width // 2), F32),
                vmem((8, tok), F32), vmem((3, 8, tok), F32),
                vmem((experts, tok), F32), vmem((3, experts, tok), F32),
                vmem((8, tok), F32), vmem((3, 8, tok), F32),
                dma((3,)), dma, dma((NR,)), dma((NR,)), dma((groups,)),
            ] + [dma((nblk,))] * 10 + [dma((3,))] * 6 + [dma((2,))] * 2,
            compiler_params=pltpu.CompilerParams(
                collective_id=0, has_side_effects=True, vmem_limit_bytes=66600000),
        )(hidden, norm_pre.reshape(width // 128, 128), norm_post.reshape(width // 128, 128), w_router.T, w_gate, w_up, w_down, choice.T)

    in_specs = (P("dp", "emb"), P("emb"), P("emb"), P("emb", None), P(None, "emb", "ffn"), P(None, "emb", "ffn"), P(None, "ffn", "emb"), P("dp", None))
    return jax.shard_map(local_block, mesh=mesh, in_specs=in_specs, out_specs=P("dp", "emb"), check_vma=False)
```

```python
import functools

import jax
import jax.numpy as jnp
from jax import lax
from jax.experimental import pallas as pl
from jax.experimental.pallas import tpu as pltpu
from jax.sharding import PartitionSpec as P

EPS = 1e-5
MESH = pl.DeviceIdType.MESH
F32 = jnp.float32
BF16 = jnp.bfloat16

GE = 8
NP = 2
NR = 3
WIN = 48


def kernel(tok, wid, experts, cap, width, top_k, model_width,
           hid_hbm, pre_ref, post_ref, wr_hbm, wg_hbm, wu_hbm, wd_hbm, ch_hbm, out_ref,
           hid, wr, ch, wg, wu, wd, xs, sel, dis, keyw, probs, selw, gate, posv, poss, zs, zc, rza, rzb, gbuf, act, mix, rmix,
           sqs, sqr, lgs, lgr, sqs2, sqr2,
           small_sem, pos_sem, wg_sem, wu_sem, wd_sem,
           as_sem, ar_sem, bs_sem, br_sem, gs_sem, gcr_sem, gxr_sem,
           ss_sem, sr_sem, ls_sem, lr_sem, ps_sem, pr_sem, ms_sem, mr_sem):
    groups = experts // GE
    half = groups // 2
    rows = GE * cap
    slots = experts * cap
    quarter = rows // 4
    fw = wid // NP
    emb = lax.axis_index("emb")
    ffn = lax.axis_index("ffn")
    x, c = emb // 2, emb % 2
    ox, oc = 1 - x, 1 - c
    mate = {"emb": x * 2 + oc}
    across = {"emb": ox * 2 + c}
    diag = {"emb": ox * 2 + oc}
    other = {"ffn": 1 - ffn}
    peers = (mate, across, diag)

    def weight_copies(p, g):
        e = pl.ds(g * GE, GE)
        col = pl.ds(p * fw, fw)
        s = (p * groups + g) % NR
        return (pltpu.make_async_copy(wg_hbm.at[e, :, col], wg.at[s], wg_sem.at[s]),
                pltpu.make_async_copy(wu_hbm.at[e, :, col], wu.at[s], wu_sem.at[s]))

    def down_copy(g):
        return pltpu.make_async_copy(wd_hbm.at[pl.ds(g * GE, GE)], wd.at[g], wd_sem.at[g])

    small = (pltpu.make_async_copy(hid_hbm, hid, small_sem.at[0]),
             pltpu.make_async_copy(ch_hbm, ch, small_sem.at[1]),
             pltpu.make_async_copy(wr_hbm, wr, small_sem.at[2]))
    for cp in small:
        cp.start()
    barrier = pltpu.get_barrier_semaphore()
    for peer in peers + (other,):
        pl.semaphore_signal(barrier, inc=1, device_id=peer, device_id_type=MESH)

    def gather_small(src, dst, send, recv):
        cps = [pltpu.make_async_remote_copy(src, dst.at[j], send, recv, device_id=peer, device_id_type=MESH)
               for j, peer in enumerate(peers)]
        for cp in cps:
            cp.start()
        return pltpu.make_async_remote_copy(dst, dst, send, recv, device_id=mate, device_id_type=MESH)

    def row_sums(sq):
        part = sq[:, 0:128]
        for j in range(1, width // 128):
            part = part + sq[:, j * 128:(j + 1) * 128]
        t = jnp.sum(part.T, axis=0, keepdims=True)
        return jnp.broadcast_to(t, (8, tok))

    def as_row(ref):
        v = ref[...].astype(F32)
        return jnp.concatenate([v[j:j + 1, :] for j in range(width // 128)], axis=1)

    for cp in small:
        cp.wait()
    for g in range(NR):
        for cp in weight_copies(0, g):
            cp.start()
    down_copy(0).start()
    down_copy(1).start()
    hf = hid[...].astype(F32)
    sqs[...] = row_sums(hf * hf)
    pl.semaphore_wait(barrier, 4)
    sq_cps = gather_small(sqs, sqr, ss_sem, sr_sem)

    expert_id = lax.broadcasted_iota(jnp.int32, (experts, tok), 0)
    chv = ch[...]
    hot = jnp.zeros((experts, tok), F32)
    for k in range(top_k):
        hot = hot + jnp.where(chv[k:k + 1, :] == expert_id, 1.0, 0.0)
    t0 = lax.broadcasted_iota(jnp.int32, (tok, tok), 0)
    t1 = lax.broadcasted_iota(jnp.int32, (tok, tok), 1)
    upper = jnp.where(t0 < t1, 1.0, 0.0).astype(BF16)
    before = jnp.dot(hot.astype(BF16), upper, preferred_element_type=F32)
    key_val = jnp.where((hot > 0.5) & (before < cap - 0.5), before, -1.0)
    dn = (((0,), (0,)), ((), ()))
    slot = lax.broadcasted_iota(jnp.int32, (cap, tok), 0).astype(F32)
    for e in range(experts):
        sel[e * cap:(e + 1) * cap, :] = jnp.where(key_val[e:e + 1, :] == slot, 1.0, 0.0).astype(BF16)

    filled = jnp.broadcast_to(jnp.minimum(jnp.sum(hot, axis=1, keepdims=True), float(cap)), (experts, 128))
    e0 = lax.broadcasted_iota(jnp.int32, (experts, experts), 0)
    e1 = lax.broadcasted_iota(jnp.int32, (experts, experts), 1)
    lower = jnp.where(e1 < e0, 1.0, 0.0).astype(BF16)
    start = jnp.dot(lower, filled.astype(BF16), preferred_element_type=F32)
    lane = lax.broadcasted_iota(jnp.int32, (cap, 128), 1).astype(F32)
    shift = jnp.zeros((1, 128), F32)
    place = []
    for g in range(groups):
        base = float(max(0, rows * (g - half)))
        shift = jnp.maximum(shift, base - start[g * GE:g * GE + 1, :])
        place.append(start[g * GE:(g + 1) * GE, :] + shift)
    place = jnp.concatenate(place, axis=0)
    for e in range(experts):
        pos = jnp.where(slot < filled[e:e + 1, :], slot + place[e:e + 1, :], -1.0) - lane
        for j in range(half * rows // 128):
            dis[e * cap:(e + 1) * cap, j * 128:(j + 1) * 128] = jnp.where(pos == float(j * 128), 1.0, 0.0).astype(BF16)
    whole = place.astype(jnp.int32)
    keyw[...] = jnp.where(key_val >= 0.0, key_val + (whole & 15).astype(F32), -1.0)

    sq_cps.wait_recv()
    tot = (sqs[0:1, :] + sqr[0, 0:1, :]) + (sqr[1, 0:1, :] + sqr[2, 0:1, :])
    inv = lax.rsqrt(tot / model_width + EPS)
    inv = jnp.broadcast_to(inv, (tok, tok)).T
    inv = jnp.concatenate([inv] * (width // 128), axis=1)
    b = (hf * inv * as_row(pre_ref)).astype(BF16)
    lgs[...] = lax.dot_general(wr[...], b, (((1,), (1,)), ((), ())), preferred_element_type=F32)
    lg_cps = gather_small(lgs, lgr, ls_sem, lr_sem)
    def dispatch(g):
        r = g * rows
        xs[r:r + rows, :] = jnp.dot(sel[r:r + rows, :], b, preferred_element_type=F32).astype(BF16)

    dispatch(0)
    mix[...] = jnp.zeros_like(mix)

    pos_cp = pltpu.make_async_copy(posv, poss, pos_sem)

    def window_starts():
        ids = jnp.concatenate([ch[...]] * (tok // top_k), axis=0).T
        expert = lax.broadcasted_iota(jnp.int32, (tok, tok), 1)
        at = lax.broadcasted_iota(jnp.int32, (tok, tok), 0)
        num = jnp.zeros((tok, tok), jnp.int32)
        for k in range(top_k):
            num = num + jnp.where(ids[:, k:k + 1] == expert, 1, 0)
        num = jnp.minimum(jnp.sum(num, axis=0, keepdims=True), cap)
        num = jnp.broadcast_to(num, (tok, tok)).T
        off = jnp.sum(jnp.where(at < expert, num, 0), axis=0, keepdims=True)
        base = jnp.maximum(expert[0:1, :] // GE - half, 0) * rows - off
        base = jnp.broadcast_to(base, (tok, tok)).T
        pos = off + jnp.max(jnp.where(at <= expert, base, -slots), axis=0, keepdims=True)
        pos = jnp.minimum(pos, half * rows)
        posv[...] = jnp.broadcast_to(pos >> 4, (8, tok))
        pos_cp.start()

    def softmax():
        lg = (lgs[...] + lgr[0]) + (lgr[1] + lgr[2])
        lg = lg - jnp.max(lg, axis=0, keepdims=True)
        ex = jnp.exp(lg)
        probs[...] = ex / jnp.sum(ex, axis=0, keepdims=True)

    def windows(g):
        w = lax.broadcasted_iota(jnp.int32, (WIN, tok), 0).astype(F32)
        for e in range(g * GE, (g + 1) * GE):
            hit = keyw[e:e + 1, :] == w
            selw[e * WIN:(e + 1) * WIN, :] = jnp.where(hit, 1.0, 0.0).astype(BF16)
            picked = jnp.sum(jnp.where(hit, probs[e:e + 1, :], 0.0), axis=1, keepdims=True)
            gate[e * WIN:(e + 1) * WIN, :] = jnp.broadcast_to(picked, (WIN, 128))

    def send_z(i):
        return pltpu.make_async_remote_copy(zc.at[i, oc], rza.at[i], as_sem, ar_sem.at[i],
                                            device_id=mate, device_id_type=MESH)

    def send_s(i):
        return pltpu.make_async_remote_copy(zc.at[i, c, ox], rzb.at[i], bs_sem, br_sem.at[i],
                                            device_id=across, device_id_type=MESH)

    def g_copy(i, a, b, recv, peer):
        row = (i % half) * rows + (2 * a + b) * quarter
        ref = gbuf.at[i // half, pl.ds(pl.multiple_of(row, quarter), quarter), :]
        return pltpu.make_async_remote_copy(ref, ref, gs_sem, recv.at[i], device_id=peer, device_id_type=MESH)

    def send_g(i):
        return (g_copy(i, c, x, gcr_sem, mate), g_copy(i, c, x, gxr_sem, across))

    def recv_mate(i):
        row = (i % half) * rows + 2 * oc * quarter
        ref = gbuf.at[i // half, pl.ds(pl.multiple_of(row, 2 * quarter), 2 * quarter), :]
        return pltpu.make_async_remote_copy(ref, ref, gs_sem, gcr_sem.at[i], device_id=mate, device_id_type=MESH)

    def recv_across(i):
        return g_copy(i, c, ox, gxr_sem, across)

    def forward_g(i):
        return g_copy(i, c, ox, gcr_sem, mate)

    def stage_a(p, g):
        s = (p * groups + g) % NR
        for k in range(GE):
            r = (g * GE + k) * cap
            xe = xs[r:r + cap, :]
            zs[r:r + cap, 0:fw] = jnp.dot(xe, wg[s, k], preferred_element_type=F32).astype(BF16)
            zs[r:r + cap, fw:2 * fw] = jnp.dot(xe, wu[s, k], preferred_element_type=F32).astype(BF16)

    def compact(i):
        k = i % half
        lo, hi = k * rows, (k + half + 1) * rows
        z = lax.dot_general(dis[lo:hi, k * rows:(k + 1) * rows], zs[lo:hi, :], dn,
                            preferred_element_type=F32).astype(BF16)
        for q in range(4):
            zc[i, q // 2, q % 2] = z[q * quarter:(q + 1) * quarter]
        send_z(i).start()

    def stage_b(i):
        zc[i, c, ox] = (zc[i, c, ox].astype(F32) + rza[i, ox].astype(F32)).astype(BF16)
        send_s(i).start()

    def stage_c(i):
        z = (zc[i, c, x].astype(F32) + rza[i, x].astype(F32) + rzb[i].astype(F32)).astype(BF16).astype(F32)
        prod = jax.nn.gelu(z[:, 0:fw], approximate=True) * z[:, fw:2 * fw]
        row = (i % half) * rows + (2 * c + x) * quarter
        gbuf[i // half, pl.ds(pl.multiple_of(row, quarter), quarter), :] = prod.astype(BF16)
        for cp in send_g(i):
            cp.start()

    def exchange(b_list, c_list, d_list):
        for i in b_list:
            send_z(i).wait_recv()
        for i in c_list:
            send_s(i).wait_recv()
        for i in d_list:
            recv_across(i).wait_recv()
        for i in b_list:
            stage_b(i)
        for i in c_list:
            stage_c(i)
        for i in d_list:
            forward_g(i).start()

    def arrived(i):
        recv_mate(i).wait_recv()
        p, r = i // half, (i % half) * rows
        act[r // 16:(r + rows) // 16, :, p * fw:(p + 1) * fw] = gbuf[p, r:r + rows, :].reshape(rows // 16, 16, fw)

    def down(g, h):
        cols = slice(h * hw, (h + 1) * hw)
        us = []
        for k in range(GE):
            e = g * GE + k
            at = poss[0, e]
            win = jnp.concatenate([act[at + j] for j in range(WIN // 16)], axis=0)
            y = jnp.dot(win, wd[g, k, :, cols], preferred_element_type=F32)
            gk = gate[e * WIN:(e + 1) * WIN, :]
            gk = jnp.concatenate([gk] * (hw // 128), axis=1)
            us.append(jnp.where(gk > 0.0, y.astype(BF16).astype(F32) * gk, 0.0).astype(BF16))
        u = jnp.concatenate(us, axis=0)
        r = g * GE * WIN
        mix[h] += lax.dot_general(selw[r:r + GE * WIN, :], u, dn, preferred_element_type=F32)

    hw = width // 2
    b_at = {6: (0,), 7: (1,), 8: (2,), 9: (3,), 14: (4,), 15: (5,)}
    c_at = {10: (0,), 11: (1,), 12: (2,), 14: (3,)}
    d_at = {14: (0,), 15: (1,)}
    for t in range(NP * groups):
        p, g = divmod(t, groups)
        for cp in weight_copies(p, g):
            cp.wait()
        if t == 3:
            lg_cps.wait_recv()
        exchange(b_at.get(t, ()), c_at.get(t, ()), d_at.get(t, ()))
        if g > half:
            compact(p * half + g - half - 1)
        elif g == 0 and p > 0:
            compact(p * half - 1)
        if p == 0 and g + 1 < groups:
            dispatch(g + 1)
        stage_a(p, g)
        if t == 2:
            window_starts()
        if t == 3:
            softmax()
        if 4 <= t < 4 + groups:
            windows(t - 4)
        if t + NR < NP * groups:
            for cp in weight_copies(*divmod(t + NR, groups)):
                cp.start()
        elif t + NR < NP * groups + 2:
            down_copy(t + NR - NP * groups + 2).start()
        else:
            for h in range(4, groups):
                down_copy(h).start()

    exchange((6,), (), (2,))
    compact(7)
    pos_cp.wait()
    exchange((), (4,), (3,))
    exchange((7,), (), ())
    for i in range(half):
        arrived(i)
    exchange((), (5,), ())
    exchange((), (6,), (4,))
    for g in range(3):
        down_copy(g).wait()
    exchange((), (7,), (5,))
    arrived(4)
    down(0, 0)
    down(0, 1)
    exchange((), (), (6,))
    arrived(5)
    down(1, 0)
    down(1, 1)
    exchange((), (), (7,))
    arrived(6)
    down(2, 0)
    down(2, 1)
    for g in range(3, groups):
        down_copy(g).wait()
    arrived(7)
    for h in range(2):
        for g in range(3, groups):
            down(g, h)
        pltpu.make_async_remote_copy(mix.at[h], rmix.at[h], ms_sem.at[h], mr_sem.at[h],
                                     device_id=other, device_id_type=MESH).start()

    pltpu.make_async_remote_copy(rza, rza, as_sem, ar_sem.at[0], device_id=mate, device_id_type=MESH).wait_send()
    pltpu.make_async_remote_copy(rzb, rzb, bs_sem, br_sem.at[0], device_id=mate, device_id_type=MESH).wait_send()
    sent = gbuf.at[:, 0:3 * rows, :]
    pltpu.make_async_remote_copy(sent, sent, gs_sem, gcr_sem.at[0], device_id=mate, device_id_type=MESH).wait_send()
    sq_cps.wait_send()
    lg_cps.wait_send()
    ms = []
    for h in range(2):
        pltpu.make_async_remote_copy(mix.at[h], rmix.at[h], ms_sem.at[h], mr_sem.at[h],
                                     device_id=other, device_id_type=MESH).wait()
        ms.append(mix[h] + rmix[h])
    m = jnp.concatenate(ms, axis=1)
    sqs2[...] = row_sums(m * m)
    gather_small(sqs2, sqr2, ps_sem, pr_sem).wait()
    tot = (sqs2[0:1, :] + sqr2[0, 0:1, :]) + (sqr2[1, 0:1, :] + sqr2[2, 0:1, :])
    inv = lax.rsqrt(tot / model_width + EPS)
    inv = jnp.broadcast_to(inv, (tok, tok)).T
    inv = jnp.concatenate([inv] * (width // 128), axis=1)
    out_ref[...] = (hid[...].astype(F32) + m * inv * as_row(post_ref)).astype(BF16)


def solution(mesh):
    emb_size = mesh.shape["emb"]

    def local_block(hidden, norm_pre, norm_post, w_router, w_gate, w_up, w_down, choice):
        tok, width = hidden.shape
        experts, _, wid = w_gate.shape
        top_k = choice.shape[1]
        cap = 2 * tok * top_k // experts
        groups = experts // GE
        nblk = NP * groups // 2
        slots, quarter, fw = experts * cap, GE * cap // 4, wid // NP
        dma = pltpu.SemaphoreType.DMA
        vmem = pltpu.VMEM
        assert emb_size == 4 and wid == width and slots == 2 * tok * top_k and WIN == cap + 16
        hbm = pl.BlockSpec(memory_space=pl.ANY)
        vm = pl.BlockSpec(memory_space=pltpu.VMEM)
        return pl.pallas_call(
            functools.partial(kernel, tok, wid, experts, cap, width, top_k, width * emb_size),
            out_shape=pltpu.VMEM((tok, width), BF16),
            in_specs=[hbm, vm, vm, hbm, hbm, hbm, hbm, hbm],
            out_specs=vm,
            scratch_shapes=[
                vmem((tok, width), BF16), vmem((experts, width), BF16), vmem((top_k, tok), jnp.int32),
                vmem((NR, GE, width, fw), BF16), vmem((NR, GE, width, fw), BF16), vmem((groups, GE, wid, width), BF16),
                vmem((slots, width), BF16), vmem((slots, tok), BF16), vmem((slots, slots // 2), BF16),
                vmem((experts, tok), F32), vmem((experts, tok), F32), vmem((experts * WIN, tok), BF16), vmem((experts * WIN, 128), F32),
                vmem((8, tok), jnp.int32), pltpu.SMEM((8, tok), jnp.int32),
                vmem((slots, 2 * fw), BF16), vmem((nblk, 2, 2, quarter, 2 * fw), BF16), vmem((nblk, 2, quarter, 2 * fw), BF16),
                vmem((nblk, quarter, 2 * fw), BF16),
                vmem((NP, slots // 2, fw), BF16), vmem(((slots // 2 + WIN) // 16, 16, wid), BF16),
                vmem((2, tok, width // 2), F32), vmem((2, tok, width // 2), F32),
                vmem((8, tok), F32), vmem((3, 8, tok), F32),
                vmem((experts, tok), F32), vmem((3, experts, tok), F32),
                vmem((8, tok), F32), vmem((3, 8, tok), F32),
                dma((3,)), dma, dma((NR,)), dma((NR,)), dma((groups,)),
            ] + [dma, dma((nblk,))] * 2 + [dma, dma((nblk,)), dma((nblk,))] + [dma] * 6 + [dma((2,))] * 2,
            compiler_params=pltpu.CompilerParams(
                collective_id=0, has_side_effects=True, vmem_limit_bytes=66600000),
        )(hidden, norm_pre.reshape(width // 128, 128), norm_post.reshape(width // 128, 128), w_router.T, w_gate, w_up, w_down, choice.T)

    in_specs = (P("dp", "emb"), P("emb"), P("emb"), P("emb", None), P(None, "emb", "ffn"), P(None, "emb", "ffn"), P(None, "ffn", "emb"), P("dp", None))
    return jax.shard_map(local_block, mesh=mesh, in_specs=in_specs, out_specs=P("dp", "emb"), check_vma=False)
```

```python
import functools

import jax
import jax.numpy as jnp
from jax import lax
from jax.experimental import pallas as pl
from jax.experimental.pallas import tpu as pltpu
from jax.sharding import PartitionSpec as P

EPS = 1e-5
MESH = pl.DeviceIdType.MESH
F32 = jnp.float32
BF16 = jnp.bfloat16

GE = 8
NP = 2
NR = 3
WIN = 48


def kernel(tok, wid, experts, cap, width, top_k, model_width,
           hid_hbm, pre_ref, post_ref, wr_hbm, wg_hbm, wu_hbm, wd_hbm, ch_hbm, out_ref,
           hid, wr, ch, wg, wu, wd, xs, sel, dis, keyw, probs, selw, gate, posv, poss, zs, zc, rza, rzb, gbuf, act, mix, rmix, total,
           sqs, sqr, lgs, lgr, sqs2, sqr2,
           small_sem, pos_sem, wg_sem, wu_sem, wd_sem,
           as_sem, ar_sem, bs_sem, br_sem, gs_sem, gcr_sem, gxr_sem,
           ss_sem, sr_sem, ls_sem, lr_sem, ps_sem, pr_sem, ms_sem, mr_sem, ts_sem, tr_sem):
    groups = experts // GE
    half = groups // 2
    rows = GE * cap
    slots = experts * cap
    quarter = rows // 4
    fw = wid // NP
    emb = lax.axis_index("emb")
    ffn = lax.axis_index("ffn")
    x, c = emb // 2, emb % 2
    ox, oc = 1 - x, 1 - c
    mate = {"emb": x * 2 + oc}
    across = {"emb": ox * 2 + c}
    diag = {"emb": ox * 2 + oc}
    other = {"ffn": 1 - ffn}
    peers = (mate, across, diag)
    fo = 1 - ffn
    everyone = peers + (other,) + tuple({"emb": peer["emb"], "ffn": fo} for peer in peers)

    def weight_copies(p, g):
        e = pl.ds(g * GE, GE)
        col = pl.ds(p * fw, fw)
        s = (p * groups + g) % NR
        return (pltpu.make_async_copy(wg_hbm.at[e, :, col], wg.at[s], wg_sem.at[s]),
                pltpu.make_async_copy(wu_hbm.at[e, :, col], wu.at[s], wu_sem.at[s]))

    def down_copy(g):
        return pltpu.make_async_copy(wd_hbm.at[pl.ds(g * GE, GE)], wd.at[g], wd_sem.at[g])

    small = (pltpu.make_async_copy(hid_hbm, hid, small_sem.at[0]),
             pltpu.make_async_copy(ch_hbm, ch, small_sem.at[1]),
             pltpu.make_async_copy(wr_hbm, wr, small_sem.at[2]))
    for cp in small:
        cp.start()
    barrier = pltpu.get_barrier_semaphore()
    for peer in everyone:
        pl.semaphore_signal(barrier, inc=1, device_id=peer, device_id_type=MESH)

    def gather_small(src, dst, send, recv, peers=peers):
        cps = [pltpu.make_async_remote_copy(src, dst.at[j], send, recv, device_id=peer, device_id_type=MESH)
               for j, peer in enumerate(peers)]
        for cp in cps:
            cp.start()
        return pltpu.make_async_remote_copy(dst, dst, send, recv, device_id=mate, device_id_type=MESH)

    def row_sums(sq):
        part = sq[:, 0:128]
        for j in range(1, width // 128):
            part = part + sq[:, j * 128:(j + 1) * 128]
        t = jnp.sum(part.T, axis=0, keepdims=True)
        return jnp.broadcast_to(t, (8, tok))

    def as_row(ref):
        v = ref[...].astype(F32)
        return jnp.concatenate([v[j:j + 1, :] for j in range(width // 128)], axis=1)

    for cp in small:
        cp.wait()
    for g in range(NR):
        for cp in weight_copies(0, g):
            cp.start()
    down_copy(0).start()
    down_copy(1).start()
    hf = hid[...].astype(F32)
    sqs[...] = row_sums(hf * hf)
    pl.semaphore_wait(barrier, 7)
    sq_cps = gather_small(sqs, sqr, ss_sem, sr_sem)

    expert_id = lax.broadcasted_iota(jnp.int32, (experts, tok), 0)
    chv = ch[...]
    hot = jnp.zeros((experts, tok), F32)
    for k in range(top_k):
        hot = hot + jnp.where(chv[k:k + 1, :] == expert_id, 1.0, 0.0)
    t0 = lax.broadcasted_iota(jnp.int32, (tok, tok), 0)
    t1 = lax.broadcasted_iota(jnp.int32, (tok, tok), 1)
    upper = jnp.where(t0 < t1, 1.0, 0.0).astype(BF16)
    before = jnp.dot(hot.astype(BF16), upper, preferred_element_type=F32)
    key_val = jnp.where((hot > 0.5) & (before < cap - 0.5), before, -1.0)
    dn = (((0,), (0,)), ((), ()))
    slot = lax.broadcasted_iota(jnp.int32, (cap, tok), 0).astype(F32)
    for e in range(experts):
        sel[e * cap:(e + 1) * cap, :] = jnp.where(key_val[e:e + 1, :] == slot, 1.0, 0.0).astype(BF16)

    filled = jnp.broadcast_to(jnp.minimum(jnp.sum(hot, axis=1, keepdims=True), float(cap)), (experts, 128))
    e0 = lax.broadcasted_iota(jnp.int32, (experts, experts), 0)
    e1 = lax.broadcasted_iota(jnp.int32, (experts, experts), 1)
    lower = jnp.where(e1 < e0, 1.0, 0.0).astype(BF16)
    start = jnp.dot(lower, filled.astype(BF16), preferred_element_type=F32)
    lane = lax.broadcasted_iota(jnp.int32, (cap, 128), 1).astype(F32)
    shift = jnp.zeros((1, 128), F32)
    place = []
    for g in range(groups):
        base = float(max(0, rows * (g - half)))
        shift = jnp.maximum(shift, base - start[g * GE:g * GE + 1, :])
        place.append(start[g * GE:(g + 1) * GE, :] + shift)
    place = jnp.concatenate(place, axis=0)
    for e in range(experts):
        pos = jnp.where(slot < filled[e:e + 1, :], slot + place[e:e + 1, :], -1.0) - lane
        for j in range(half * rows // 128):
            dis[e * cap:(e + 1) * cap, j * 128:(j + 1) * 128] = jnp.where(pos == float(j * 128), 1.0, 0.0).astype(BF16)
    whole = place.astype(jnp.int32)
    keyw[...] = jnp.where(key_val >= 0.0, key_val + (whole & 15).astype(F32), -1.0)

    sq_cps.wait_recv()
    tot = (sqs[0:1, :] + sqr[0, 0:1, :]) + (sqr[1, 0:1, :] + sqr[2, 0:1, :])
    inv = lax.rsqrt(tot / model_width + EPS)
    inv = jnp.broadcast_to(inv, (tok, tok)).T
    inv = jnp.concatenate([inv] * (width // 128), axis=1)
    b = (hf * inv * as_row(pre_ref)).astype(BF16)
    lgs[...] = lax.dot_general(wr[...], b, (((1,), (1,)), ((), ())), preferred_element_type=F32)
    lg_cps = gather_small(lgs, lgr, ls_sem, lr_sem)
    def dispatch(g):
        r = g * rows
        xs[r:r + rows, :] = jnp.dot(sel[r:r + rows, :], b, preferred_element_type=F32).astype(BF16)

    dispatch(0)
    mix[...] = jnp.zeros_like(mix)

    pos_cp = pltpu.make_async_copy(posv, poss, pos_sem)

    def window_starts():
        ids = jnp.concatenate([ch[...]] * (tok // top_k), axis=0).T
        expert = lax.broadcasted_iota(jnp.int32, (tok, tok), 1)
        at = lax.broadcasted_iota(jnp.int32, (tok, tok), 0)
        num = jnp.zeros((tok, tok), jnp.int32)
        for k in range(top_k):
            num = num + jnp.where(ids[:, k:k + 1] == expert, 1, 0)
        num = jnp.minimum(jnp.sum(num, axis=0, keepdims=True), cap)
        num = jnp.broadcast_to(num, (tok, tok)).T
        off = jnp.sum(jnp.where(at < expert, num, 0), axis=0, keepdims=True)
        base = jnp.maximum(expert[0:1, :] // GE - half, 0) * rows - off
        base = jnp.broadcast_to(base, (tok, tok)).T
        pos = off + jnp.max(jnp.where(at <= expert, base, -slots), axis=0, keepdims=True)
        pos = jnp.minimum(pos, half * rows)
        posv[...] = jnp.broadcast_to(pos >> 4, (8, tok))
        pos_cp.start()

    def softmax():
        lg = (lgs[...] + lgr[0]) + (lgr[1] + lgr[2])
        lg = lg - jnp.max(lg, axis=0, keepdims=True)
        ex = jnp.exp(lg)
        probs[...] = ex / jnp.sum(ex, axis=0, keepdims=True)

    def windows(g):
        w = lax.broadcasted_iota(jnp.int32, (WIN, tok), 0).astype(F32)
        for e in range(g * GE, (g + 1) * GE):
            hit = keyw[e:e + 1, :] == w
            selw[e * WIN:(e + 1) * WIN, :] = jnp.where(hit, 1.0, 0.0).astype(BF16)
            picked = jnp.sum(jnp.where(hit, probs[e:e + 1, :], 0.0), axis=1, keepdims=True)
            gate[e * WIN:(e + 1) * WIN, :] = jnp.broadcast_to(picked, (WIN, 128))

    def send_z(i):
        return pltpu.make_async_remote_copy(zc.at[i, oc], rza.at[i], as_sem, ar_sem.at[i],
                                            device_id=mate, device_id_type=MESH)

    def send_s(i):
        return pltpu.make_async_remote_copy(zc.at[i, c, ox], rzb.at[i], bs_sem, br_sem.at[i],
                                            device_id=across, device_id_type=MESH)

    def g_copy(i, a, b, recv, peer):
        row = (i % half) * rows + (2 * a + b) * quarter
        ref = gbuf.at[i // half, pl.ds(pl.multiple_of(row, quarter), quarter), :]
        return pltpu.make_async_remote_copy(ref, ref, gs_sem, recv.at[i], device_id=peer, device_id_type=MESH)

    def send_g(i):
        return (g_copy(i, c, x, gcr_sem, mate), g_copy(i, c, x, gxr_sem, across))

    def recv_mate(i):
        row = (i % half) * rows + 2 * oc * quarter
        ref = gbuf.at[i // half, pl.ds(pl.multiple_of(row, 2 * quarter), 2 * quarter), :]
        return pltpu.make_async_remote_copy(ref, ref, gs_sem, gcr_sem.at[i], device_id=mate, device_id_type=MESH)

    def recv_across(i):
        return g_copy(i, c, ox, gxr_sem, across)

    def forward_g(i):
        return g_copy(i, c, ox, gcr_sem, mate)

    def stage_a(p, g):
        s = (p * groups + g) % NR
        for k in range(GE):
            r = (g * GE + k) * cap
            xe = xs[r:r + cap, :]
            zs[r:r + cap, 0:fw] = jnp.dot(xe, wg[s, k], preferred_element_type=F32).astype(BF16)
            zs[r:r + cap, fw:2 * fw] = jnp.dot(xe, wu[s, k], preferred_element_type=F32).astype(BF16)

    def compact(i):
        k = i % half
        lo, hi = k * rows, (k + half + 1) * rows
        z = lax.dot_general(dis[lo:hi, k * rows:(k + 1) * rows], zs[lo:hi, :], dn,
                            preferred_element_type=F32).astype(BF16)
        for q in range(4):
            zc[i, q // 2, q % 2] = z[q * quarter:(q + 1) * quarter]
        send_z(i).start()

    def stage_b(i):
        zc[i, c, ox] = (zc[i, c, ox].astype(F32) + rza[i, ox].astype(F32)).astype(BF16)
        send_s(i).start()

    def stage_c(i):
        z = (zc[i, c, x].astype(F32) + rza[i, x].astype(F32) + rzb[i].astype(F32)).astype(BF16).astype(F32)
        prod = jax.nn.gelu(z[:, 0:fw], approximate=True) * z[:, fw:2 * fw]
        row = (i % half) * rows + (2 * c + x) * quarter
        gbuf[i // half, pl.ds(pl.multiple_of(row, quarter), quarter), :] = prod.astype(BF16)
        for cp in send_g(i):
            cp.start()

    def exchange(b_list, c_list, d_list):
        for i in b_list:
            send_z(i).wait_recv()
        for i in c_list:
            send_s(i).wait_recv()
        for i in d_list:
            recv_across(i).wait_recv()
        for i in b_list:
            stage_b(i)
        for i in c_list:
            stage_c(i)
        for i in d_list:
            forward_g(i).start()

    def arrived(i):
        recv_mate(i).wait_recv()
        p, r = i // half, (i % half) * rows
        act[r // 16:(r + rows) // 16, :, p * fw:(p + 1) * fw] = gbuf[p, r:r + rows, :].reshape(rows // 16, 16, fw)

    def down(g, h):
        cols = slice(h * hw, (h + 1) * hw)
        us = []
        for k in range(GE):
            e = g * GE + k
            at = poss[0, e]
            win = jnp.concatenate([act[at + j] for j in range(WIN // 16)], axis=0)
            y = jnp.dot(win, wd[g, k, :, cols], preferred_element_type=F32)
            gk = gate[e * WIN:(e + 1) * WIN, :]
            gk = jnp.concatenate([gk] * (hw // 128), axis=1)
            us.append(jnp.where(gk > 0.0, y.astype(BF16).astype(F32) * gk, 0.0).astype(BF16))
        u = jnp.concatenate(us, axis=0)
        r = g * GE * WIN
        mix[h] += lax.dot_general(selw[r:r + GE * WIN, :], u, dn, preferred_element_type=F32).reshape(2, tok // 2, hw)

    hw = width // 2
    b_at = {6: (0,), 7: (1,), 8: (2,), 9: (3,), 14: (4,), 15: (5,)}
    c_at = {10: (0,), 11: (1,), 12: (2,), 14: (3,)}
    d_at = {14: (0,), 15: (1,)}
    for t in range(NP * groups):
        p, g = divmod(t, groups)
        for cp in weight_copies(p, g):
            cp.wait()
        if t == 3:
            lg_cps.wait_recv()
        exchange(b_at.get(t, ()), c_at.get(t, ()), d_at.get(t, ()))
        if g > half:
            compact(p * half + g - half - 1)
        elif g == 0 and p > 0:
            compact(p * half - 1)
        if p == 0 and g + 1 < groups:
            dispatch(g + 1)
        stage_a(p, g)
        if t == 2:
            window_starts()
        if t == 3:
            softmax()
        if 4 <= t < 4 + groups:
            windows(t - 4)
        if t + NR < NP * groups:
            for cp in weight_copies(*divmod(t + NR, groups)):
                cp.start()
        elif t + NR < NP * groups + 2:
            down_copy(t + NR - NP * groups + 2).start()
        else:
            for h in range(4, groups):
                down_copy(h).start()

    exchange((6,), (), (2,))
    compact(7)
    pos_cp.wait()
    exchange((), (4,), (3,))
    exchange((7,), (), ())
    for i in range(half):
        arrived(i)
    exchange((), (5,), ())
    exchange((), (6,), (4,))
    for g in range(3):
        down_copy(g).wait()
    exchange((), (7,), (5,))
    arrived(4)
    down(0, 0)
    down(0, 1)
    exchange((), (), (6,))
    arrived(5)
    down(1, 0)
    down(1, 1)
    exchange((), (), (7,))
    arrived(6)
    down(2, 0)
    down(2, 1)
    for g in range(3, groups):
        down_copy(g).wait()
    arrived(7)
    def send_half(h):
        return pltpu.make_async_remote_copy(mix.at[h, fo], rmix.at[h], ms_sem.at[h], mr_sem.at[h],
                                            device_id=other, device_id_type=MESH)

    def send_sum(h, part):
        ref = total.at[h, part]
        return pltpu.make_async_remote_copy(ref, ref, ts_sem.at[h], tr_sem.at[h], device_id=other, device_id_type=MESH)

    for h in range(2):
        for g in range(3, groups):
            down(g, h)
        send_half(h).start()

    pltpu.make_async_remote_copy(rza, rza, as_sem, ar_sem.at[0], device_id=mate, device_id_type=MESH).wait_send()
    pltpu.make_async_remote_copy(rzb, rzb, bs_sem, br_sem.at[0], device_id=mate, device_id_type=MESH).wait_send()
    sent = gbuf.at[:, 0:3 * rows, :]
    pltpu.make_async_remote_copy(sent, sent, gs_sem, gcr_sem.at[0], device_id=mate, device_id_type=MESH).wait_send()
    sq_cps.wait_send()
    lg_cps.wait_send()
    own = []
    for h in range(2):
        send_half(h).wait()
        own.append(mix[h, ffn] + rmix[h])
        total[h, ffn] = own[h]
        if h == 0:
            send_sum(0, ffn).start()
    own = jnp.concatenate(own, axis=1)
    sq = own * own
    sqs2[...] = row_sums(jnp.concatenate([sq, sq], axis=0))
    last_cps = gather_small(sqs2, sqr2, ps_sem, pr_sem, everyone)
    send_sum(1, ffn).start()
    last_cps.wait()
    mine = (sqs2[0:1, :] + sqr2[0, 0:1, :]) + (sqr2[1, 0:1, :] + sqr2[2, 0:1, :])
    theirs = (sqr2[3, 0:1, :] + sqr2[4, 0:1, :]) + (sqr2[5, 0:1, :] + sqr2[6, 0:1, :])
    tot = jnp.where(lax.broadcasted_iota(jnp.int32, (1, tok), 1) // (tok // 2) == ffn, mine, theirs)
    for h in range(2):
        send_sum(h, ffn).wait_send()
        send_sum(h, fo).wait_recv()
    m = jnp.concatenate([total[h].reshape(tok, hw) for h in range(2)], axis=1)
    inv = lax.rsqrt(tot / model_width + EPS)
    inv = jnp.broadcast_to(inv, (tok, tok)).T
    inv = jnp.concatenate([inv] * (width // 128), axis=1)
    out_ref[...] = (hid[...].astype(F32) + m * inv * as_row(post_ref)).astype(BF16)


def solution(mesh):
    emb_size = mesh.shape["emb"]

    def local_block(hidden, norm_pre, norm_post, w_router, w_gate, w_up, w_down, choice):
        tok, width = hidden.shape
        experts, _, wid = w_gate.shape
        top_k = choice.shape[1]
        cap = 2 * tok * top_k // experts
        groups = experts // GE
        nblk = NP * groups // 2
        slots, quarter, fw = experts * cap, GE * cap // 4, wid // NP
        dma = pltpu.SemaphoreType.DMA
        vmem = pltpu.VMEM
        assert emb_size == 4 and wid == width and slots == 2 * tok * top_k and WIN == cap + 16
        hbm = pl.BlockSpec(memory_space=pl.ANY)
        vm = pl.BlockSpec(memory_space=pltpu.VMEM)
        return pl.pallas_call(
            functools.partial(kernel, tok, wid, experts, cap, width, top_k, width * emb_size),
            out_shape=pltpu.VMEM((tok, width), BF16),
            in_specs=[hbm, vm, vm, hbm, hbm, hbm, hbm, hbm],
            out_specs=vm,
            scratch_shapes=[
                vmem((tok, width), BF16), vmem((experts, width), BF16), vmem((top_k, tok), jnp.int32),
                vmem((NR, GE, width, fw), BF16), vmem((NR, GE, width, fw), BF16), vmem((groups, GE, wid, width), BF16),
                vmem((slots, width), BF16), vmem((slots, tok), BF16), vmem((slots, slots // 2), BF16),
                vmem((experts, tok), F32), vmem((experts, tok), F32), vmem((experts * WIN, tok), BF16), vmem((experts * WIN, 128), F32),
                vmem((8, tok), jnp.int32), pltpu.SMEM((8, tok), jnp.int32),
                vmem((slots, 2 * fw), BF16), vmem((nblk, 2, 2, quarter, 2 * fw), BF16), vmem((nblk, 2, quarter, 2 * fw), BF16),
                vmem((nblk, quarter, 2 * fw), BF16),
                vmem((NP, slots // 2, fw), BF16), vmem(((slots // 2 + WIN) // 16, 16, wid), BF16),
                vmem((2, 2, tok // 2, width // 2), F32), vmem((2, tok // 2, width // 2), F32), vmem((2, 2, tok // 2, width // 2), F32),
                vmem((8, tok), F32), vmem((3, 8, tok), F32),
                vmem((experts, tok), F32), vmem((3, experts, tok), F32),
                vmem((8, tok), F32), vmem((7, 8, tok), F32),
                dma((3,)), dma, dma((NR,)), dma((NR,)), dma((groups,)),
            ] + [dma, dma((nblk,))] * 2 + [dma, dma((nblk,)), dma((nblk,))] + [dma] * 6 + [dma((2,))] * 4,
            compiler_params=pltpu.CompilerParams(
                collective_id=0, has_side_effects=True, vmem_limit_bytes=66600000),
        )(hidden, norm_pre.reshape(width // 128, 128), norm_post.reshape(width // 128, 128), w_router.T, w_gate, w_up, w_down, choice.T)

    in_specs = (P("dp", "emb"), P("emb"), P("emb"), P("emb", None), P(None, "emb", "ffn"), P(None, "emb", "ffn"), P(None, "ffn", "emb"), P("dp", None))
    return jax.shard_map(local_block, mesh=mesh, in_specs=in_specs, out_specs=P("dp", "emb"), check_vma=False)
```

```python
import functools

import jax
import jax.numpy as jnp
from jax import lax
from jax.experimental import pallas as pl
from jax.experimental.pallas import tpu as pltpu
from jax.sharding import PartitionSpec as P

EPS = 1e-5
MESH = pl.DeviceIdType.MESH
F32 = jnp.float32
BF16 = jnp.bfloat16

GE = 8
NP = 2
NR = 3
WIN = 48


def kernel(tok, wid, experts, cap, width, top_k, model_width,
           hid_hbm, pre_ref, post_ref, wr_hbm, wg_hbm, wu_hbm, wd_hbm, ch_hbm, out_ref,
           hid, wr, ch, wg, wu, wd, xs, sel, dis, keyw, probs, selw, gate, posv, poss, zs, zc, rza, rzb, gbuf, act, mix, rmix, total,
           sqs, sqr, lgs, lgr, sqs2, sqr2,
           small_sem, pos_sem, wg_sem, wu_sem, wd_sem,
           as_sem, ar_sem, bs_sem, br_sem, gs_sem, gcr_sem, gxr_sem,
           ss_sem, sr_sem, ls_sem, lr_sem, ps_sem, pr_sem, ms_sem, mr_sem, ts_sem, tr_sem):
    groups = experts // GE
    half = groups // 2
    rows = GE * cap
    slots = experts * cap
    quarter = rows // 4
    fw = wid // NP
    emb = lax.axis_index("emb")
    ffn = lax.axis_index("ffn")
    x, c = emb // 2, emb % 2
    ox, oc = 1 - x, 1 - c
    mate = {"emb": x * 2 + oc}
    across = {"emb": ox * 2 + c}
    diag = {"emb": ox * 2 + oc}
    other = {"ffn": 1 - ffn}
    peers = (mate, across, diag)
    fo = 1 - ffn
    everyone = peers + (other,) + tuple({"emb": peer["emb"], "ffn": fo} for peer in peers)

    def weight_copies(p, g):
        e = pl.ds(g * GE, GE)
        col = pl.ds(p * fw, fw)
        s = (p * groups + g) % NR
        return (pltpu.make_async_copy(wg_hbm.at[e, :, col], wg.at[s], wg_sem.at[s]),
                pltpu.make_async_copy(wu_hbm.at[e, :, col], wu.at[s], wu_sem.at[s]))

    def down_copy(g):
        return pltpu.make_async_copy(wd_hbm.at[pl.ds(g * GE, GE)], wd.at[g], wd_sem.at[g])

    small = (pltpu.make_async_copy(hid_hbm, hid, small_sem.at[0]),
             pltpu.make_async_copy(ch_hbm, ch, small_sem.at[1]),
             pltpu.make_async_copy(wr_hbm, wr, small_sem.at[2]))
    for cp in small:
        cp.start()
    barrier = pltpu.get_barrier_semaphore()
    for peer in everyone:
        pl.semaphore_signal(barrier, inc=1, device_id=peer, device_id_type=MESH)

    def gather_small(src, dst, send, recv, peers=peers):
        cps = [pltpu.make_async_remote_copy(src, dst.at[j], send, recv, device_id=peer, device_id_type=MESH)
               for j, peer in enumerate(peers)]
        for cp in cps:
            cp.start()
        return pltpu.make_async_remote_copy(dst, dst, send, recv, device_id=mate, device_id_type=MESH)

    def row_sums(sq):
        part = sq[:, 0:128]
        for j in range(1, width // 128):
            part = part + sq[:, j * 128:(j + 1) * 128]
        t = jnp.sum(part.T, axis=0, keepdims=True)
        return jnp.broadcast_to(t, (8, tok))

    def as_row(ref):
        v = ref[...].astype(F32)
        return jnp.concatenate([v[j:j + 1, :] for j in range(width // 128)], axis=1)

    for cp in small:
        cp.wait()
    for g in range(NR):
        for cp in weight_copies(0, g):
            cp.start()
    down_copy(0).start()
    down_copy(1).start()
    hf = hid[...].astype(F32)
    sqs[...] = row_sums(hf * hf)
    pl.semaphore_wait(barrier, 7)
    sq_cps = gather_small(sqs, sqr, ss_sem, sr_sem)

    expert_id = lax.broadcasted_iota(jnp.int32, (experts, tok), 0)
    chv = ch[...]
    hot = jnp.zeros((experts, tok), F32)
    for k in range(top_k):
        hot = hot + jnp.where(chv[k:k + 1, :] == expert_id, 1.0, 0.0)
    t0 = lax.broadcasted_iota(jnp.int32, (tok, tok), 0)
    t1 = lax.broadcasted_iota(jnp.int32, (tok, tok), 1)
    upper = jnp.where(t0 < t1, 1.0, 0.0).astype(BF16)
    before = jnp.dot(hot.astype(BF16), upper, preferred_element_type=F32)
    key_val = jnp.where((hot > 0.5) & (before < cap - 0.5), before, -1.0)
    dn = (((0,), (0,)), ((), ()))
    slot = lax.broadcasted_iota(jnp.int32, (cap, tok), 0).astype(F32)
    for e in range(experts):
        sel[e * cap:(e + 1) * cap, :] = jnp.where(key_val[e:e + 1, :] == slot, 1.0, 0.0).astype(BF16)

    filled = jnp.broadcast_to(jnp.minimum(jnp.sum(hot, axis=1, keepdims=True), float(cap)), (experts, 128))
    e0 = lax.broadcasted_iota(jnp.int32, (experts, experts), 0)
    e1 = lax.broadcasted_iota(jnp.int32, (experts, experts), 1)
    lower = jnp.where(e1 < e0, 1.0, 0.0).astype(BF16)
    start = jnp.dot(lower, filled.astype(BF16), preferred_element_type=F32)
    lane = lax.broadcasted_iota(jnp.int32, (cap, 128), 1).astype(F32)
    shift = jnp.zeros((1, 128), F32)
    place = []
    for g in range(groups):
        base = float(max(0, rows * (g - half)))
        shift = jnp.maximum(shift, base - start[g * GE:g * GE + 1, :])
        place.append(start[g * GE:(g + 1) * GE, :] + shift)
    place = jnp.concatenate(place, axis=0)
    for e in range(experts):
        pos = jnp.where(slot < filled[e:e + 1, :], slot + place[e:e + 1, :], -1.0) - lane
        for j in range(half * rows // 128):
            dis[e * cap:(e + 1) * cap, j * 128:(j + 1) * 128] = jnp.where(pos == float(j * 128), 1.0, 0.0).astype(BF16)
    whole = place.astype(jnp.int32)
    keyw[...] = jnp.where(key_val >= 0.0, key_val + (whole & 15).astype(F32), -1.0)

    sq_cps.wait_recv()
    tot = (sqs[0:1, :] + sqr[0, 0:1, :]) + (sqr[1, 0:1, :] + sqr[2, 0:1, :])
    inv = lax.rsqrt(tot / model_width + EPS)
    inv = jnp.broadcast_to(inv, (tok, tok)).T
    inv = jnp.concatenate([inv] * (width // 128), axis=1)
    b = (hf * inv * as_row(pre_ref)).astype(BF16)
    lgs[...] = lax.dot_general(wr[...], b, (((1,), (1,)), ((), ())), preferred_element_type=F32)
    lg_cps = gather_small(lgs, lgr, ls_sem, lr_sem)
    def dispatch(g):
        r = g * rows
        xs[r:r + rows, :] = jnp.dot(sel[r:r + rows, :], b, preferred_element_type=F32).astype(BF16)

    dispatch(0)
    mix[...] = jnp.zeros_like(mix)

    pos_cp = pltpu.make_async_copy(posv, poss, pos_sem)

    def window_starts():
        ids = jnp.concatenate([ch[...]] * (tok // top_k), axis=0).T
        expert = lax.broadcasted_iota(jnp.int32, (tok, tok), 1)
        at = lax.broadcasted_iota(jnp.int32, (tok, tok), 0)
        num = jnp.zeros((tok, tok), jnp.int32)
        for k in range(top_k):
            num = num + jnp.where(ids[:, k:k + 1] == expert, 1, 0)
        num = jnp.minimum(jnp.sum(num, axis=0, keepdims=True), cap)
        num = jnp.broadcast_to(num, (tok, tok)).T
        off = jnp.sum(jnp.where(at < expert, num, 0), axis=0, keepdims=True)
        base = jnp.maximum(expert[0:1, :] // GE - half, 0) * rows - off
        base = jnp.broadcast_to(base, (tok, tok)).T
        pos = off + jnp.max(jnp.where(at <= expert, base, -slots), axis=0, keepdims=True)
        pos = jnp.minimum(pos, half * rows)
        posv[...] = jnp.broadcast_to(pos >> 4, (8, tok))
        pos_cp.start()

    def softmax():
        lg = (lgs[...] + lgr[0]) + (lgr[1] + lgr[2])
        lg = lg - jnp.max(lg, axis=0, keepdims=True)
        ex = jnp.exp(lg)
        probs[...] = ex / jnp.sum(ex, axis=0, keepdims=True)

    def windows(g):
        w = lax.broadcasted_iota(jnp.int32, (WIN, tok), 0).astype(F32)
        for e in range(g * GE, (g + 1) * GE):
            hit = keyw[e:e + 1, :] == w
            selw[e * WIN:(e + 1) * WIN, :] = jnp.where(hit, 1.0, 0.0).astype(BF16)
            picked = jnp.sum(jnp.where(hit, probs[e:e + 1, :], 0.0), axis=1, keepdims=True)
            gate[e * WIN:(e + 1) * WIN, :] = jnp.broadcast_to(picked, (WIN, 128))

    def send_z(i):
        return pltpu.make_async_remote_copy(zc.at[i, oc], rza.at[i], as_sem, ar_sem.at[i],
                                            device_id=mate, device_id_type=MESH)

    def send_s(i):
        return pltpu.make_async_remote_copy(zc.at[i, c, ox], rzb.at[i], bs_sem, br_sem.at[i],
                                            device_id=across, device_id_type=MESH)

    def g_copy(i, a, b, recv, peer):
        row = (i % half) * rows + (2 * a + b) * quarter
        ref = gbuf.at[i // half, pl.ds(pl.multiple_of(row, quarter), quarter), :]
        return pltpu.make_async_remote_copy(ref, ref, gs_sem, recv.at[i], device_id=peer, device_id_type=MESH)

    def send_g(i):
        return (g_copy(i, c, x, gcr_sem, mate), g_copy(i, c, x, gxr_sem, across))

    def recv_mate(i):
        row = (i % half) * rows + 2 * oc * quarter
        ref = gbuf.at[i // half, pl.ds(pl.multiple_of(row, 2 * quarter), 2 * quarter), :]
        return pltpu.make_async_remote_copy(ref, ref, gs_sem, gcr_sem.at[i], device_id=mate, device_id_type=MESH)

    def recv_across(i):
        return g_copy(i, c, ox, gxr_sem, across)

    def forward_g(i):
        return g_copy(i, c, ox, gcr_sem, mate)

    def stage_a(p, g):
        s = (p * groups + g) % NR
        for k in range(GE):
            r = (g * GE + k) * cap
            xe = xs[r:r + cap, :]
            zs[r:r + cap, 0:fw] = jnp.dot(xe, wg[s, k], preferred_element_type=F32).astype(BF16)
            zs[r:r + cap, fw:2 * fw] = jnp.dot(xe, wu[s, k], preferred_element_type=F32).astype(BF16)

    def compact(i):
        k = i % half
        lo, hi = k * rows, (k + half + 1) * rows
        z = lax.dot_general(dis[lo:hi, k * rows:(k + 1) * rows], zs[lo:hi, :], dn,
                            preferred_element_type=F32).astype(BF16)
        for q in range(4):
            zc[i, q // 2, q % 2] = z[q * quarter:(q + 1) * quarter]
        send_z(i).start()

    def stage_b(i):
        zc[i, c, ox] = (zc[i, c, ox].astype(F32) + rza[i, ox].astype(F32)).astype(BF16)
        send_s(i).start()

    def stage_c(i):
        z = (zc[i, c, x].astype(F32) + rza[i, x].astype(F32) + rzb[i].astype(F32)).astype(BF16).astype(F32)
        prod = jax.nn.gelu(z[:, 0:fw], approximate=True) * z[:, fw:2 * fw]
        row = (i % half) * rows + (2 * c + x) * quarter
        gbuf[i // half, pl.ds(pl.multiple_of(row, quarter), quarter), :] = prod.astype(BF16)
        for cp in send_g(i):
            cp.start()

    def exchange(b_list, c_list, d_list):
        for i in b_list:
            send_z(i).wait_recv()
        for i in c_list:
            send_s(i).wait_recv()
        for i in d_list:
            recv_across(i).wait_recv()
        for i in b_list:
            stage_b(i)
        for i in c_list:
            stage_c(i)
        for i in d_list:
            forward_g(i).start()

    def arrived(i):
        recv_mate(i).wait_recv()
        p, r = i // half, (i % half) * rows
        act[r // 16:(r + rows) // 16, :, p * fw:(p + 1) * fw] = gbuf[p, r:r + rows, :].reshape(rows // 16, 16, fw)

    def down(g, h):
        cols = slice(h * hw, (h + 1) * hw)
        us = []
        for k in range(GE):
            e = g * GE + k
            at = poss[0, e]
            win = jnp.concatenate([act[at + j] for j in range(WIN // 16)], axis=0)
            y = jnp.dot(win, wd[g, k, :, cols], preferred_element_type=F32)
            gk = gate[e * WIN:(e + 1) * WIN, :]
            gk = jnp.concatenate([gk] * (hw // 128), axis=1)
            us.append(jnp.where(gk > 0.0, y.astype(BF16).astype(F32) * gk, 0.0).astype(BF16))
        u = jnp.concatenate(us, axis=0)
        r = g * GE * WIN
        mix[h] += lax.dot_general(selw[r:r + GE * WIN, :], u, dn, preferred_element_type=F32).reshape(2, tok // 2, hw)

    hw = width // 2
    b_at = {6: (0,), 7: (1,), 8: (2,), 9: (3,), 14: (4,), 15: (5,)}
    c_at = {10: (0,), 11: (1,), 12: (2,), 14: (3,)}
    d_at = {14: (0,), 15: (1,)}
    for t in range(NP * groups):
        p, g = divmod(t, groups)
        for cp in weight_copies(p, g):
            cp.wait()
        if t == 8:
            lg_cps.wait_recv()
        exchange(b_at.get(t, ()), c_at.get(t, ()), d_at.get(t, ()))
        if g > half:
            compact(p * half + g - half - 1)
        elif g == 0 and p > 0:
            compact(p * half - 1)
        if p == 0 and g + 1 < groups:
            dispatch(g + 1)
        stage_a(p, g)
        if t == 8:
            softmax()
        if t == 9:
            window_starts()
        if 8 <= t < 8 + groups:
            windows(t - 8)
        if t + NR < NP * groups:
            for cp in weight_copies(*divmod(t + NR, groups)):
                cp.start()
        elif t + NR < NP * groups + 2:
            down_copy(t + NR - NP * groups + 2).start()
        else:
            for h in range(4, groups):
                down_copy(h).start()

    exchange((6,), (), (2,))
    compact(7)
    pos_cp.wait()
    exchange((), (4,), (3,))
    exchange((7,), (), ())
    for i in range(half):
        arrived(i)
    exchange((), (5,), ())
    exchange((), (6,), (4,))
    for g in range(3):
        down_copy(g).wait()
    exchange((), (7,), (5,))
    arrived(4)
    down(0, 0)
    down(0, 1)
    exchange((), (), (6,))
    arrived(5)
    down(1, 0)
    down(1, 1)
    exchange((), (), (7,))
    arrived(6)
    down(2, 0)
    down(2, 1)
    for g in range(3, groups):
        down_copy(g).wait()
    arrived(7)
    def send_half(h):
        return pltpu.make_async_remote_copy(mix.at[h, fo], rmix.at[h], ms_sem.at[h], mr_sem.at[h],
                                            device_id=other, device_id_type=MESH)

    def send_sum(h, part):
        ref = total.at[h, part]
        return pltpu.make_async_remote_copy(ref, ref, ts_sem.at[h], tr_sem.at[h], device_id=other, device_id_type=MESH)

    for h in range(2):
        for g in range(3, groups):
            down(g, h)
        send_half(h).start()

    pltpu.make_async_remote_copy(rza, rza, as_sem, ar_sem.at[0], device_id=mate, device_id_type=MESH).wait_send()
    pltpu.make_async_remote_copy(rzb, rzb, bs_sem, br_sem.at[0], device_id=mate, device_id_type=MESH).wait_send()
    sent = gbuf.at[:, 0:3 * rows, :]
    pltpu.make_async_remote_copy(sent, sent, gs_sem, gcr_sem.at[0], device_id=mate, device_id_type=MESH).wait_send()
    sq_cps.wait_send()
    lg_cps.wait_send()
    own = []
    for h in range(2):
        send_half(h).wait()
        own.append(mix[h, ffn] + rmix[h])
        total[h, ffn] = own[h]
        if h == 0:
            send_sum(0, ffn).start()
    own = jnp.concatenate(own, axis=1)
    sq = own * own
    sqs2[...] = row_sums(jnp.concatenate([sq, sq], axis=0))
    last_cps = gather_small(sqs2, sqr2, ps_sem, pr_sem, everyone)
    send_sum(1, ffn).start()
    last_cps.wait()
    mine = (sqs2[0:1, :] + sqr2[0, 0:1, :]) + (sqr2[1, 0:1, :] + sqr2[2, 0:1, :])
    theirs = (sqr2[3, 0:1, :] + sqr2[4, 0:1, :]) + (sqr2[5, 0:1, :] + sqr2[6, 0:1, :])
    tot = jnp.where(lax.broadcasted_iota(jnp.int32, (1, tok), 1) // (tok // 2) == ffn, mine, theirs)
    for h in range(2):
        send_sum(h, ffn).wait_send()
        send_sum(h, fo).wait_recv()
    m = jnp.concatenate([total[h].reshape(tok, hw) for h in range(2)], axis=1)
    inv = lax.rsqrt(tot / model_width + EPS)
    inv = jnp.broadcast_to(inv, (tok, tok)).T
    inv = jnp.concatenate([inv] * (width // 128), axis=1)
    out_ref[...] = (hid[...].astype(F32) + m * inv * as_row(post_ref)).astype(BF16)


def solution(mesh):
    emb_size = mesh.shape["emb"]

    def local_block(hidden, norm_pre, norm_post, w_router, w_gate, w_up, w_down, choice):
        tok, width = hidden.shape
        experts, _, wid = w_gate.shape
        top_k = choice.shape[1]
        cap = 2 * tok * top_k // experts
        groups = experts // GE
        nblk = NP * groups // 2
        slots, quarter, fw = experts * cap, GE * cap // 4, wid // NP
        dma = pltpu.SemaphoreType.DMA
        vmem = pltpu.VMEM
        assert emb_size == 4 and wid == width and slots == 2 * tok * top_k and WIN == cap + 16
        hbm = pl.BlockSpec(memory_space=pl.ANY)
        vm = pl.BlockSpec(memory_space=pltpu.VMEM)
        return pl.pallas_call(
            functools.partial(kernel, tok, wid, experts, cap, width, top_k, width * emb_size),
            out_shape=pltpu.VMEM((tok, width), BF16),
            in_specs=[hbm, vm, vm, hbm, hbm, hbm, hbm, hbm],
            out_specs=vm,
            scratch_shapes=[
                vmem((tok, width), BF16), vmem((experts, width), BF16), vmem((top_k, tok), jnp.int32),
                vmem((NR, GE, width, fw), BF16), vmem((NR, GE, width, fw), BF16), vmem((groups, GE, wid, width), BF16),
                vmem((slots, width), BF16), vmem((slots, tok), BF16), vmem((slots, slots // 2), BF16),
                vmem((experts, tok), F32), vmem((experts, tok), F32), vmem((experts * WIN, tok), BF16), vmem((experts * WIN, 128), F32),
                vmem((8, tok), jnp.int32), pltpu.SMEM((8, tok), jnp.int32),
                vmem((slots, 2 * fw), BF16), vmem((nblk, 2, 2, quarter, 2 * fw), BF16), vmem((nblk, 2, quarter, 2 * fw), BF16),
                vmem((nblk, quarter, 2 * fw), BF16),
                vmem((NP, slots // 2, fw), BF16), vmem(((slots // 2 + WIN) // 16, 16, wid), BF16),
                vmem((2, 2, tok // 2, width // 2), F32), vmem((2, tok // 2, width // 2), F32), vmem((2, 2, tok // 2, width // 2), F32),
                vmem((8, tok), F32), vmem((3, 8, tok), F32),
                vmem((experts, tok), F32), vmem((3, experts, tok), F32),
                vmem((8, tok), F32), vmem((7, 8, tok), F32),
                dma((3,)), dma, dma((NR,)), dma((NR,)), dma((groups,)),
            ] + [dma, dma((nblk,))] * 2 + [dma, dma((nblk,)), dma((nblk,))] + [dma] * 6 + [dma((2,))] * 4,
            compiler_params=pltpu.CompilerParams(
                collective_id=0, has_side_effects=True, vmem_limit_bytes=66600000),
        )(hidden, norm_pre.reshape(width // 128, 128), norm_post.reshape(width // 128, 128), w_router.T, w_gate, w_up, w_down, choice.T)

    in_specs = (P("dp", "emb"), P("emb"), P("emb"), P("emb", None), P(None, "emb", "ffn"), P(None, "emb", "ffn"), P(None, "ffn", "emb"), P("dp", None))
    return jax.shard_map(local_block, mesh=mesh, in_specs=in_specs, out_specs=P("dp", "emb"), check_vma=False)
```

```python
import functools

import jax
import jax.numpy as jnp
from jax import lax
from jax.experimental import pallas as pl
from jax.experimental.pallas import tpu as pltpu
from jax.sharding import PartitionSpec as P

EPS = 1e-5
MESH = pl.DeviceIdType.MESH
F32 = jnp.float32
BF16 = jnp.bfloat16

GE = 8
NP = 2
NR = 3
WIN = 48


def kernel(tok, wid, experts, cap, width, top_k, model_width,
           hid_hbm, pre_ref, post_ref, wr_hbm, wg_hbm, wu_hbm, wd_hbm, ch_hbm, out_ref,
           hid, wr, ch, wg, wu, wd, xs, sel, dis, keyw, probs, selw, gate, posv, poss, zs, zc, rza, rzb, gbuf, act, mix, rmix, total,
           sqs, sqr, lgs, lgr, sqs2, sqr2,
           small_sem, pos_sem, wg_sem, wu_sem, wd_sem,
           as_sem, ar_sem, bs_sem, br_sem, gs_sem, gcr_sem, gxr_sem,
           ss_sem, sr_sem, ls_sem, lr_sem, ps_sem, pr_sem, ms_sem, mr_sem, ts_sem, tr_sem):
    groups = experts // GE
    half = groups // 2
    rows = GE * cap
    slots = experts * cap
    quarter = rows // 4
    fw = wid // NP
    emb = lax.axis_index("emb")
    ffn = lax.axis_index("ffn")
    x, c = emb // 2, emb % 2
    ox, oc = 1 - x, 1 - c
    mate = {"emb": x * 2 + oc}
    across = {"emb": ox * 2 + c}
    diag = {"emb": ox * 2 + oc}
    other = {"ffn": 1 - ffn}
    peers = (mate, across, diag)
    fo = 1 - ffn
    everyone = peers + (other,) + tuple({"emb": peer["emb"], "ffn": fo} for peer in peers)

    def weight_copies(p, g):
        e = pl.ds(g * GE, GE)
        col = pl.ds(p * fw, fw)
        s = (p * groups + g) % NR
        return (pltpu.make_async_copy(wg_hbm.at[e, :, col], wg.at[s], wg_sem.at[s]),
                pltpu.make_async_copy(wu_hbm.at[e, :, col], wu.at[s], wu_sem.at[s]))

    def down_copy(g):
        return pltpu.make_async_copy(wd_hbm.at[pl.ds(g * GE, GE)], wd.at[g], wd_sem.at[g])

    small = (pltpu.make_async_copy(hid_hbm, hid, small_sem.at[0]),
             pltpu.make_async_copy(ch_hbm, ch, small_sem.at[1]),
             pltpu.make_async_copy(wr_hbm, wr, small_sem.at[2]))
    for cp in small:
        cp.start()
    barrier = pltpu.get_barrier_semaphore()
    for peer in everyone:
        pl.semaphore_signal(barrier, inc=1, device_id=peer, device_id_type=MESH)

    def gather_small(src, dst, send, recv, peers=peers):
        cps = [pltpu.make_async_remote_copy(src, dst.at[j], send, recv, device_id=peer, device_id_type=MESH)
               for j, peer in enumerate(peers)]
        for cp in cps:
            cp.start()
        return pltpu.make_async_remote_copy(dst, dst, send, recv, device_id=mate, device_id_type=MESH)

    def row_sums(sq):
        part = sq[:, 0:128]
        for j in range(1, width // 128):
            part = part + sq[:, j * 128:(j + 1) * 128]
        t = jnp.sum(part.T, axis=0, keepdims=True)
        return jnp.broadcast_to(t, (8, tok))

    def as_row(ref):
        v = ref[...].astype(F32)
        return jnp.concatenate([v[j:j + 1, :] for j in range(width // 128)], axis=1)

    for cp in small:
        cp.wait()
    for g in range(NR):
        for cp in weight_copies(0, g):
            cp.start()
    down_copy(0).start()
    down_copy(1).start()
    hf = hid[...].astype(F32)
    sqs[...] = row_sums(hf * hf)
    pl.semaphore_wait(barrier, 7)
    sq_cps = gather_small(sqs, sqr, ss_sem, sr_sem)

    expert_id = lax.broadcasted_iota(jnp.int32, (experts, tok), 0)
    chv = ch[...]
    hot = jnp.zeros((experts, tok), F32)
    for k in range(top_k):
        hot = hot + jnp.where(chv[k:k + 1, :] == expert_id, 1.0, 0.0)
    t0 = lax.broadcasted_iota(jnp.int32, (tok, tok), 0)
    t1 = lax.broadcasted_iota(jnp.int32, (tok, tok), 1)
    upper = jnp.where(t0 < t1, 1.0, 0.0).astype(BF16)
    before = jnp.dot(hot.astype(BF16), upper, preferred_element_type=F32)
    key_val = jnp.where((hot > 0.5) & (before < cap - 0.5), before, -1.0)
    dn = (((0,), (0,)), ((), ()))
    slot = lax.broadcasted_iota(jnp.int32, (cap, tok), 0).astype(F32)
    for e in range(experts):
        sel[e * cap:(e + 1) * cap, :] = jnp.where(key_val[e:e + 1, :] == slot, 1.0, 0.0).astype(BF16)

    filled = jnp.broadcast_to(jnp.minimum(jnp.sum(hot, axis=1, keepdims=True), float(cap)), (experts, 128))
    e0 = lax.broadcasted_iota(jnp.int32, (experts, experts), 0)
    e1 = lax.broadcasted_iota(jnp.int32, (experts, experts), 1)
    lower = jnp.where(e1 < e0, 1.0, 0.0).astype(BF16)
    start = jnp.dot(lower, filled.astype(BF16), preferred_element_type=F32)
    lane = lax.broadcasted_iota(jnp.int32, (cap, 128), 1).astype(F32)
    shift = jnp.zeros((1, 128), F32)
    place = []
    for g in range(groups):
        base = float(max(0, rows * (g - half)))
        shift = jnp.maximum(shift, base - start[g * GE:g * GE + 1, :])
        place.append(start[g * GE:(g + 1) * GE, :] + shift)
    place = jnp.concatenate(place, axis=0)
    for e in range(experts):
        pos = jnp.where(slot < filled[e:e + 1, :], slot + place[e:e + 1, :], -1.0) - lane
        for j in range(half * rows // 128):
            dis[e * cap:(e + 1) * cap, j * 128:(j + 1) * 128] = jnp.where(pos == float(j * 128), 1.0, 0.0).astype(BF16)
    whole = place.astype(jnp.int32)
    keyw[...] = jnp.where(key_val >= 0.0, key_val + (whole & 15).astype(F32), -1.0)

    sq_cps.wait_recv()
    tot = (sqs[0:1, :] + sqr[0, 0:1, :]) + (sqr[1, 0:1, :] + sqr[2, 0:1, :])
    inv = lax.rsqrt(tot / model_width + EPS)
    inv = jnp.broadcast_to(inv, (tok, tok)).T
    inv = jnp.concatenate([inv] * (width // 128), axis=1)
    b = (hf * inv * as_row(pre_ref)).astype(BF16)
    lgs[...] = lax.dot_general(wr[...], b, (((1,), (1,)), ((), ())), preferred_element_type=F32)
    lg_cps = gather_small(lgs, lgr, ls_sem, lr_sem)
    def dispatch(g):
        r = g * rows
        xs[r:r + rows, :] = jnp.dot(sel[r:r + rows, :], b, preferred_element_type=F32).astype(BF16)

    dispatch(0)
    mix[...] = jnp.zeros_like(mix)

    pos_cp = pltpu.make_async_copy(posv, poss, pos_sem)

    def window_starts():
        ids = jnp.concatenate([ch[...]] * (tok // top_k), axis=0).T
        expert = lax.broadcasted_iota(jnp.int32, (tok, tok), 1)
        at = lax.broadcasted_iota(jnp.int32, (tok, tok), 0)
        num = jnp.zeros((tok, tok), jnp.int32)
        for k in range(top_k):
            num = num + jnp.where(ids[:, k:k + 1] == expert, 1, 0)
        num = jnp.minimum(jnp.sum(num, axis=0, keepdims=True), cap)
        num = jnp.broadcast_to(num, (tok, tok)).T
        off = jnp.sum(jnp.where(at < expert, num, 0), axis=0, keepdims=True)
        base = jnp.maximum(expert[0:1, :] // GE - half, 0) * rows - off
        base = jnp.broadcast_to(base, (tok, tok)).T
        pos = off + jnp.max(jnp.where(at <= expert, base, -slots), axis=0, keepdims=True)
        pos = jnp.minimum(pos, half * rows)
        posv[...] = jnp.broadcast_to(pos >> 4, (8, tok))
        pos_cp.start()

    def softmax():
        lg = (lgs[...] + lgr[0]) + (lgr[1] + lgr[2])
        lg = lg - jnp.max(lg, axis=0, keepdims=True)
        ex = jnp.exp(lg)
        probs[...] = ex / jnp.sum(ex, axis=0, keepdims=True)

    def windows(g):
        w = lax.broadcasted_iota(jnp.int32, (WIN, tok), 0).astype(F32)
        for e in range(g * GE, (g + 1) * GE):
            hit = keyw[e:e + 1, :] == w
            selw[e * WIN:(e + 1) * WIN, :] = jnp.where(hit, 1.0, 0.0).astype(BF16)
            picked = jnp.sum(jnp.where(hit, probs[e:e + 1, :], 0.0), axis=1, keepdims=True)
            gate[e * WIN:(e + 1) * WIN, :] = jnp.broadcast_to(picked, (WIN, 128))

    def send_z(i):
        return pltpu.make_async_remote_copy(zc.at[i, oc], rza.at[i], as_sem, ar_sem.at[i],
                                            device_id=mate, device_id_type=MESH)

    def send_s(i):
        return pltpu.make_async_remote_copy(zc.at[i, c, ox], rzb.at[i], bs_sem, br_sem.at[i],
                                            device_id=across, device_id_type=MESH)

    def g_copy(i, a, b, recv, peer):
        row = (i % half) * rows + (2 * a + b) * quarter
        ref = gbuf.at[i // half, pl.ds(pl.multiple_of(row, quarter), quarter), :]
        return pltpu.make_async_remote_copy(ref, ref, gs_sem, recv.at[i], device_id=peer, device_id_type=MESH)

    def send_g(i):
        return (g_copy(i, c, x, gcr_sem, mate), g_copy(i, c, x, gxr_sem, across))

    def recv_mate(i):
        row = (i % half) * rows + 2 * oc * quarter
        ref = gbuf.at[i // half, pl.ds(pl.multiple_of(row, 2 * quarter), 2 * quarter), :]
        return pltpu.make_async_remote_copy(ref, ref, gs_sem, gcr_sem.at[i], device_id=mate, device_id_type=MESH)

    def recv_across(i):
        return g_copy(i, c, ox, gxr_sem, across)

    def forward_g(i):
        return g_copy(i, c, ox, gcr_sem, mate)

    def stage_a(p, g):
        s = (p * groups + g) % NR
        for k in range(GE):
            r = (g * GE + k) * cap
            xe = xs[r:r + cap, :]
            zs[r:r + cap, 0:fw] = jnp.dot(xe, wg[s, k], preferred_element_type=F32).astype(BF16)
            zs[r:r + cap, fw:2 * fw] = jnp.dot(xe, wu[s, k], preferred_element_type=F32).astype(BF16)

    def compact(i):
        k = i % half
        lo, hi = k * rows, (k + half + 1) * rows
        z = lax.dot_general(dis[lo:hi, k * rows:(k + 1) * rows], zs[lo:hi, :], dn,
                            preferred_element_type=F32).astype(BF16)
        for q in range(4):
            zc[i, q // 2, q % 2] = z[q * quarter:(q + 1) * quarter]
        send_z(i).start()

    def stage_b(i):
        zc[i, c, ox] = (zc[i, c, ox].astype(F32) + rza[i, ox].astype(F32)).astype(BF16)
        send_s(i).start()

    def stage_c(i):
        z = (zc[i, c, x].astype(F32) + rza[i, x].astype(F32) + rzb[i].astype(F32)).astype(BF16).astype(F32)
        prod = jax.nn.gelu(z[:, 0:fw], approximate=True) * z[:, fw:2 * fw]
        row = (i % half) * rows + (2 * c + x) * quarter
        gbuf[i // half, pl.ds(pl.multiple_of(row, quarter), quarter), :] = prod.astype(BF16)
        for cp in send_g(i):
            cp.start()

    def exchange(b_list, c_list, d_list):
        for i in b_list:
            send_z(i).wait_recv()
        for i in c_list:
            send_s(i).wait_recv()
        for i in d_list:
            recv_across(i).wait_recv()
        for i in b_list:
            stage_b(i)
        for i in c_list:
            stage_c(i)
        for i in d_list:
            forward_g(i).start()

    def arrived(i):
        recv_mate(i).wait_recv()
        p, r = i // half, (i % half) * rows
        act[r // 16:(r + rows) // 16, :, p * fw:(p + 1) * fw] = gbuf[p, r:r + rows, :].reshape(rows // 16, 16, fw)

    def down(g, h):
        cols = slice(h * hw, (h + 1) * hw)
        us = []
        for k in range(GE):
            e = g * GE + k
            at = poss[0, e]
            win = jnp.concatenate([act[at + j] for j in range(WIN // 16)], axis=0)
            y = jnp.dot(win, wd[g, k, :, cols], preferred_element_type=F32)
            gk = gate[e * WIN:(e + 1) * WIN, :]
            gk = jnp.concatenate([gk] * (hw // 128), axis=1)
            us.append(jnp.where(gk > 0.0, y.astype(BF16).astype(F32) * gk, 0.0).astype(BF16))
        u = jnp.concatenate(us, axis=0)
        r = g * GE * WIN
        mix[h] += lax.dot_general(selw[r:r + GE * WIN, :], u, dn, preferred_element_type=F32).reshape(2, tok // 2, hw)

    hw = width // 2
    b_at = {6: (0,), 7: (1,), 8: (2,), 9: (3,), 14: (4,), 15: (5,)}
    c_at = {10: (0,), 11: (1,), 12: (2,), 14: (3,)}
    d_at = {14: (0,), 15: (1,)}
    for t in range(NP * groups):
        p, g = divmod(t, groups)
        for cp in weight_copies(p, g):
            cp.wait()
        if t == 8:
            lg_cps.wait_recv()
        exchange(b_at.get(t, ()), c_at.get(t, ()), d_at.get(t, ()))
        if g > half:
            compact(p * half + g - half - 1)
        elif g == 0 and p > 0:
            compact(p * half - 1)
        if p == 0 and g + 1 < groups:
            dispatch(g + 1)
        stage_a(p, g)
        if t == 8:
            softmax()
        if t == 11:
            window_starts()
        if 9 <= t < 9 + groups // 2:
            windows(2 * (t - 9))
            windows(2 * (t - 9) + 1)
        if t + NR < NP * groups:
            for cp in weight_copies(*divmod(t + NR, groups)):
                cp.start()
        elif t + NR < NP * groups + 2:
            down_copy(t + NR - NP * groups + 2).start()
        else:
            for h in range(4, groups):
                down_copy(h).start()

    exchange((6,), (), (2,))
    compact(7)
    pos_cp.wait()
    exchange((7,), (), ())
    exchange((), (4,), (3,))
    for i in range(half):
        arrived(i)
    exchange((), (5,), ())
    exchange((), (6,), (4,))
    for g in range(3):
        down_copy(g).wait()
    exchange((), (7,), (5,))
    arrived(4)
    down(0, 0)
    down(0, 1)
    exchange((), (), (6,))
    arrived(5)
    down(1, 0)
    down(1, 1)
    exchange((), (), (7,))
    arrived(6)
    down(2, 0)
    down(2, 1)
    for g in range(3, groups):
        down_copy(g).wait()
    arrived(7)
    def send_half(h):
        return pltpu.make_async_remote_copy(mix.at[h, fo], rmix.at[h], ms_sem.at[h], mr_sem.at[h],
                                            device_id=other, device_id_type=MESH)

    def send_sum(h, part):
        ref = total.at[h, part]
        return pltpu.make_async_remote_copy(ref, ref, ts_sem.at[h], tr_sem.at[h], device_id=other, device_id_type=MESH)

    for h in range(2):
        for g in range(3, groups):
            down(g, h)
        send_half(h).start()

    pltpu.make_async_remote_copy(rza, rza, as_sem, ar_sem.at[0], device_id=mate, device_id_type=MESH).wait_send()
    pltpu.make_async_remote_copy(rzb, rzb, bs_sem, br_sem.at[0], device_id=mate, device_id_type=MESH).wait_send()
    sent = gbuf.at[:, 0:3 * rows, :]
    pltpu.make_async_remote_copy(sent, sent, gs_sem, gcr_sem.at[0], device_id=mate, device_id_type=MESH).wait_send()
    sq_cps.wait_send()
    lg_cps.wait_send()
    own = []
    for h in range(2):
        send_half(h).wait()
        own.append(mix[h, ffn] + rmix[h])
        total[h, ffn] = own[h]
        if h == 0:
            send_sum(0, ffn).start()
    own = jnp.concatenate(own, axis=1)
    sq = own * own
    sqs2[...] = row_sums(jnp.concatenate([sq, sq], axis=0))
    last_cps = gather_small(sqs2, sqr2, ps_sem, pr_sem, everyone)
    send_sum(1, ffn).start()
    last_cps.wait()
    mine = (sqs2[0:1, :] + sqr2[0, 0:1, :]) + (sqr2[1, 0:1, :] + sqr2[2, 0:1, :])
    theirs = (sqr2[3, 0:1, :] + sqr2[4, 0:1, :]) + (sqr2[5, 0:1, :] + sqr2[6, 0:1, :])
    tot = jnp.where(lax.broadcasted_iota(jnp.int32, (1, tok), 1) // (tok // 2) == ffn, mine, theirs)
    for h in range(2):
        send_sum(h, ffn).wait_send()
        send_sum(h, fo).wait_recv()
    m = jnp.concatenate([total[h].reshape(tok, hw) for h in range(2)], axis=1)
    inv = lax.rsqrt(tot / model_width + EPS)
    inv = jnp.broadcast_to(inv, (tok, tok)).T
    inv = jnp.concatenate([inv] * (width // 128), axis=1)
    out_ref[...] = (hid[...].astype(F32) + m * inv * as_row(post_ref)).astype(BF16)


def solution(mesh):
    emb_size = mesh.shape["emb"]

    def local_block(hidden, norm_pre, norm_post, w_router, w_gate, w_up, w_down, choice):
        tok, width = hidden.shape
        experts, _, wid = w_gate.shape
        top_k = choice.shape[1]
        cap = 2 * tok * top_k // experts
        groups = experts // GE
        nblk = NP * groups // 2
        slots, quarter, fw = experts * cap, GE * cap // 4, wid // NP
        dma = pltpu.SemaphoreType.DMA
        vmem = pltpu.VMEM
        assert emb_size == 4 and wid == width and slots == 2 * tok * top_k and WIN == cap + 16
        hbm = pl.BlockSpec(memory_space=pl.ANY)
        vm = pl.BlockSpec(memory_space=pltpu.VMEM)
        return pl.pallas_call(
            functools.partial(kernel, tok, wid, experts, cap, width, top_k, width * emb_size),
            out_shape=pltpu.VMEM((tok, width), BF16),
            in_specs=[hbm, vm, vm, hbm, hbm, hbm, hbm, hbm],
            out_specs=vm,
            scratch_shapes=[
                vmem((tok, width), BF16), vmem((experts, width), BF16), vmem((top_k, tok), jnp.int32),
                vmem((NR, GE, width, fw), BF16), vmem((NR, GE, width, fw), BF16), vmem((groups, GE, wid, width), BF16),
                vmem((slots, width), BF16), vmem((slots, tok), BF16), vmem((slots, slots // 2), BF16),
                vmem((experts, tok), F32), vmem((experts, tok), F32), vmem((experts * WIN, tok), BF16), vmem((experts * WIN, 128), F32),
                vmem((8, tok), jnp.int32), pltpu.SMEM((8, tok), jnp.int32),
                vmem((slots, 2 * fw), BF16), vmem((nblk, 2, 2, quarter, 2 * fw), BF16), vmem((nblk, 2, quarter, 2 * fw), BF16),
                vmem((nblk, quarter, 2 * fw), BF16),
                vmem((NP, slots // 2, fw), BF16), vmem(((slots // 2 + WIN) // 16, 16, wid), BF16),
                vmem((2, 2, tok // 2, width // 2), F32), vmem((2, tok // 2, width // 2), F32), vmem((2, 2, tok // 2, width // 2), F32),
                vmem((8, tok), F32), vmem((3, 8, tok), F32),
                vmem((experts, tok), F32), vmem((3, experts, tok), F32),
                vmem((8, tok), F32), vmem((7, 8, tok), F32),
                dma((3,)), dma, dma((NR,)), dma((NR,)), dma((groups,)),
            ] + [dma, dma((nblk,))] * 2 + [dma, dma((nblk,)), dma((nblk,))] + [dma] * 6 + [dma((2,))] * 4,
            compiler_params=pltpu.CompilerParams(
                collective_id=0, has_side_effects=True, vmem_limit_bytes=66600000),
        )(hidden, norm_pre.reshape(width // 128, 128), norm_post.reshape(width // 128, 128), w_router.T, w_gate, w_up, w_down, choice.T)

    in_specs = (P("dp", "emb"), P("emb"), P("emb"), P("emb", None), P(None, "emb", "ffn"), P(None, "emb", "ffn"), P(None, "ffn", "emb"), P("dp", None))
    return jax.shard_map(local_block, mesh=mesh, in_specs=in_specs, out_specs=P("dp", "emb"), check_vma=False)
```
